256 devices in a mesh: dp: 8 (over z), expert: 4 (over y), tensor: 8 (over x, core).
Axes of the slice: x: 4, y: 4, z: 8, core: 2. Of those that a mesh axis runs over, the one named last changes fastest.
Arguments:
- tokens: bfloat16 [1024, 6144], P('dp', 'tensor'), may hold values from -6 to 6
- out_grad: bfloat16 [1024, 6144], P('dp', 'tensor'), may hold values from -6 to 6
- router_weight: bfloat16 [6144, 4], P('tensor'), may hold values from -0.078125 to 0.078125
- gate_weight: bfloat16 [4, 6144, 8192], P('expert', 'tensor', 'dp'), may hold values from -0.078125 to 0.078125
- up_weight: bfloat16 [4, 6144, 8192], P('expert', 'tensor', 'dp'), may hold values from -0.078125 to 0.078125
- down_weight: bfloat16 [4, 8192, 6144], P('expert', 'dp', 'tensor'), may hold values from -0.0625 to 0.0625
- expert_index: int32 [1024, 2], P('dp'), may hold values from 0 to 3, as said below
- slot_index: int32 [1024, 2], P('dp'), may hold values from 0 to 95, as said below
Outputs:
- tokens_grad: bfloat16 [1024, 6144], P(('dp', 'expert'), 'tensor')
- router_grad: float32 [6144, 4], P('tensor')
- gate_grad: bfloat16 [4, 6144, 8192], P('expert', 'tensor', 'dp')
- up_grad: bfloat16 [4, 6144, 8192], P('expert', 'tensor', 'dp')
- down_grad: bfloat16 [4, 8192, 6144], P('expert', 'dp', 'tensor')
The draws below stay inside these ranges and needn't reach their ends.
Inputs may be any that keep to these rules, and one draw needn't show every extreme that they name: `expert_index`: each row names two different experts; in each aligned block of 128 rows no expert is named more than 96 times, and one expert is named exactly 96 times in every block. `slot_index`: entry k of a row is a slot of the expert in entry k of the same row of expert_index; within one aligned block of 128 rows the choices of one expert have distinct slots.
All inputs are finite; a program needn't handle non-finite values.
Results may differ from the reference program's by a relative error of at most 0.025.
Values may be sent and summed in bfloat16 or wider, within the bound.
A program may use at most 64 MiB of HBM per device.

```python
from functools import partial
import jax
import jax.numpy as jnp
from jax import lax

D = 6144
FF = 8192
EXPERTS = 4
TOK_DEV = 128
CAP = 96
TOKENS = 1024
SLOTS = 768
N_TENSOR = 8


def routing_block(block_key, busiest):
    load_key, order_key, token_key, swap_key, slot_key = jax.random.split(block_key, 5)
    shares = jax.random.randint(load_key, (EXPERTS - 1,), 1, 4)
    rest_picks = 2 * TOK_DEV - CAP
    other_loads = rest_picks * shares // jnp.sum(shares)
    leftover = rest_picks - jnp.sum(other_loads)
    other_loads = other_loads.at[jnp.argmin(shares)].add(leftover)
    others = (busiest + 1 + jax.random.permutation(order_key, EXPERTS - 1)) % EXPERTS
    expert_order = jnp.concatenate([jnp.reshape(busiest, (1,)), others]).astype(jnp.int32)
    run_counts = jnp.concatenate([jnp.array([CAP], jnp.int32), other_loads.astype(jnp.int32)])
    run_ends = jnp.cumsum(run_counts)
    run_starts = run_ends - run_counts
    pick_ids = jnp.arange(2 * TOK_DEV, dtype=jnp.int32)
    pick_run = jnp.sum((pick_ids[:, None] >= run_ends[None, :]).astype(jnp.int32), axis=1)
    pick_expert = expert_order[pick_run]
    pick_offset = pick_ids - run_starts[pick_run]
    tables = jax.vmap(partial(jax.random.permutation, x=CAP))(jax.random.split(slot_key, EXPERTS))
    pick_slot = tables[pick_expert, pick_offset]
    token_order = jax.random.permutation(token_key, TOK_DEV)
    first_pick = token_order
    second_pick = token_order + TOK_DEV
    expert_pair = jnp.stack([pick_expert[first_pick], pick_expert[second_pick]], axis=1)
    slot_pair = jnp.stack([pick_slot[first_pick], pick_slot[second_pick]], axis=1)
    swap_pair = jax.random.randint(swap_key, (TOK_DEV, 1), 0, 2) == 1
    expert_pair = jnp.where(swap_pair, expert_pair[:, ::-1], expert_pair)
    slot_pair = jnp.where(swap_pair, slot_pair[:, ::-1], slot_pair)
    return (expert_pair, slot_pair)


def make_routes(key):
    base_key = jax.random.fold_in(key, 7)
    row_blocks = TOKENS // TOK_DEV
    busiest = jax.random.randint(jax.random.fold_in(base_key, 1), (), 0, EXPERTS).astype(jnp.int32)
    block_keys = jax.random.split(jax.random.fold_in(base_key, 2), row_blocks)
    expert_pair, slot_pair = jax.vmap(partial(routing_block, busiest=busiest))(block_keys)
    return (expert_pair.reshape(TOKENS, 2).astype(jnp.int32), slot_pair.reshape(TOKENS, 2).astype(jnp.int32))


def draw_expert_index(key, part):
    return make_routes(key)[0]


def draw_slot_index(key, part):
    return make_routes(key)[1]


def shard_levels(stream_key, dims, cuts, smallest, largest):
    loudness = 1.0
    for position, parts in cuts:
        heights = jax.random.uniform(jax.random.fold_in(jax.random.fold_in(stream_key, 6), position), (parts,), jnp.float32, smallest / len(cuts), largest / len(cuts))
        loudness = loudness * jnp.repeat(jnp.exp(heights), dims[position] // parts).reshape((-1,) + (1,) * (len(dims) - 1 - position))
    return loudness


def normal_values(stream_key, dims, scale, reach, pieces=(), kind=jnp.bfloat16):
    entries = scale * jax.random.normal(stream_key, dims, jnp.float32)
    if pieces:
        entries = entries * shard_levels(stream_key, dims, pieces, -0.22, 0.18)
    return jnp.clip(entries, -reach, reach).astype(kind)


def setup_inputs(seed: int = 0) -> dict:
    key_list = jax.random.split(jax.random.key(seed), 9)
    tokens = normal_values(key_list[0], (TOKENS, D), 1.0, 6.0, ((0, 8), (1, 8)))
    out_grad = normal_values(key_list[1], (TOKENS, D), 1.0, 6.0, ((0, 8), (1, 8)))
    router_weight = normal_values(key_list[2], (D, EXPERTS), D ** -0.5, 0.078125, ((0, 8),))
    gate_weight = normal_values(key_list[3], (EXPERTS, D, FF), D ** -0.5, 0.078125, ((0, 4), (1, 8), (2, 8)))
    up_weight = normal_values(key_list[4], (EXPERTS, D, FF), D ** -0.5, 0.078125, ((0, 4), (1, 8), (2, 8)))
    down_weight = normal_values(key_list[5], (EXPERTS, FF, D), FF ** -0.5, 0.0625, ((0, 4), (1, 8), (2, 8)))
    expert_index = draw_expert_index(jax.random.fold_in(key_list[8], 71), 0)
    slot_index = draw_slot_index(jax.random.fold_in(key_list[8], 71), 0)
    return dict(tokens=tokens, out_grad=out_grad, router_weight=router_weight, gate_weight=gate_weight, up_weight=up_weight, down_weight=down_weight, expert_index=expert_index, slot_index=slot_index)


highest = lax.Precision.HIGHEST


def block_sum(left_side, right_side):
    block_width = D // N_TENSOR
    running = jnp.zeros((left_side.shape[0], right_side.shape[1]), jnp.float32)
    for row_block in range(N_TENSOR):
        partial_value = jnp.dot(left_side[:, row_block * block_width:(row_block + 1) * block_width], right_side[row_block * block_width:(row_block + 1) * block_width], preferred_element_type=jnp.float32)
        partial_value = lax.optimization_barrier(partial_value.astype(jnp.bfloat16)).astype(jnp.float32)
        running = running + partial_value
    return running


def expert_backward(operands):
    slot_tokens, slot_grads, slot_prob, gate_w, up_w, down_w = operands
    gate_sum = block_sum(slot_tokens, gate_w)
    up_sum = block_sum(slot_tokens, up_w)
    grad_act = block_sum(slot_grads, down_w.T)
    gate_sigmoid = jax.nn.sigmoid(gate_sum)
    hidden = (gate_sum * gate_sigmoid * up_sum).astype(jnp.bfloat16)
    prob_grad = jnp.sum(hidden.astype(jnp.float32) * grad_act, axis=1)
    act_grad = slot_prob.astype(jnp.float32)[:, None] * grad_act
    grad_gate = (act_grad * up_sum * gate_sigmoid * (1.0 + gate_sum * (1.0 - gate_sigmoid))).astype(jnp.bfloat16)
    grad_up = (act_grad * gate_sum * gate_sigmoid).astype(jnp.bfloat16)
    scaled_grads = (slot_prob.astype(jnp.float32)[:, None] * slot_grads.astype(jnp.float32)).astype(jnp.bfloat16)
    down_grad = jnp.dot(hidden.T, scaled_grads, preferred_element_type=jnp.float32).astype(jnp.bfloat16)
    gate_grad = jnp.dot(slot_tokens.T, grad_gate, preferred_element_type=jnp.float32).astype(jnp.bfloat16)
    up_grad = jnp.dot(slot_tokens.T, grad_up, preferred_element_type=jnp.float32).astype(jnp.bfloat16)
    slot_dx = jnp.dot(grad_gate, gate_w.T, preferred_element_type=jnp.float32) + jnp.dot(grad_up, up_w.T, preferred_element_type=jnp.float32)
    return slot_dx, prob_grad, gate_grad, up_grad, down_grad


def reference(tokens, out_grad, router_weight, gate_weight, up_weight, down_weight, expert_index, slot_index):
    logits = jnp.dot(tokens, router_weight, preferred_element_type=jnp.float32)
    chosen = jnp.take_along_axis(logits, expert_index, axis=1)
    pick_prob = jnp.stack([jax.nn.sigmoid(chosen[:, 0] - chosen[:, 1]), jax.nn.sigmoid(chosen[:, 1] - chosen[:, 0])], axis=1)
    prob_low = pick_prob.astype(jnp.bfloat16)
    row_block = (jnp.arange(TOKENS, dtype=jnp.int32) // TOK_DEV).astype(jnp.int32)
    slot_place = ((expert_index * (TOKENS // TOK_DEV) + row_block[:, None]) * CAP + slot_index).astype(jnp.int32)
    flat_place = slot_place.reshape(-1)
    slot_tokens = jnp.zeros((EXPERTS * SLOTS, D), jnp.bfloat16).at[flat_place].set(jnp.repeat(tokens, 2, axis=0))
    slot_grads = jnp.zeros((EXPERTS * SLOTS, D), jnp.bfloat16).at[flat_place].set(jnp.repeat(out_grad, 2, axis=0))
    slot_prob = jnp.zeros((EXPERTS * SLOTS,), jnp.bfloat16).at[flat_place].set(prob_low.reshape(-1))
    slot_dx, prob_grad, gate_grad, up_grad, down_grad = lax.map(expert_backward, (slot_tokens.reshape(EXPERTS, SLOTS, D), slot_grads.reshape(EXPERTS, SLOTS, D), slot_prob.reshape(EXPERTS, SLOTS), gate_weight, up_weight, down_weight))
    pick_dx = slot_dx.reshape(EXPERTS * SLOTS, D)[slot_place]
    pick_grad = prob_grad.reshape(-1)[slot_place]
    mixed_grad = jnp.sum(pick_prob * pick_grad, axis=1, keepdims=True)
    weights = pick_prob * (pick_grad - mixed_grad)
    onehot = (expert_index[:, :, None] == jnp.arange(EXPERTS, dtype=jnp.int32)[None, None, :]).astype(jnp.float32)
    logit_grad = jnp.sum(onehot * weights[:, :, None], axis=1)
    tokens_grad = (jnp.sum(pick_dx, axis=1) + jnp.dot(logit_grad, router_weight.astype(jnp.float32).T, precision=highest)).astype(jnp.bfloat16)
    router_grad = jnp.dot(tokens.astype(jnp.float32).T, logit_grad, precision=highest)
    return tokens_grad, router_grad, gate_grad, up_grad, down_grad
```

```python
import jax
import jax.numpy as jnp
from jax import lax
from jax.experimental import pallas as pl
from jax.experimental.pallas import tpu as pltpu
from jax.sharding import PartitionSpec as P

CAP = 96
MESH = pl.DeviceIdType.MESH
F32 = jnp.float32
BF16 = jnp.bfloat16

ORDER = (0, -1, 1, -2, 2, 4, -3, 3)
GROUPS = (1, 2, 2, 1, 2)
POS = {o: i for i, o in enumerate(ORDER)}


def place(offset):
    o = offset % 8
    return POS[o if o <= 4 else o - 8]


CHUNKS = []
_at = 0
for _n in GROUPS:
    CHUNKS.append((_at, _n))
    _at += _n

STAGES = ("F", "R1", "R2", "E", "G1", "G2", "X")
SKEW = 2


def plan():
    steps = []
    last = len(STAGES) + SKEW * (len(CHUNKS) - 1)
    for s in range(last):
        for k in range(len(CHUNKS)):
            i = s - SKEW * k
            if 0 <= i < len(STAGES):
                steps.append((STAGES[i], k))
    return steps


def dot_nt(a, b):
    return lax.dot_general(a, b, (((1,), (1,)), ((), ())), preferred_element_type=F32)


def dot_nn(a, b):
    return lax.dot_general(a, b, (((1,), (0,)), ((), ())), preferred_element_type=F32)


class Copies:
    def __init__(self, send, recv):
        self.send, self.recv, self.count, self.made = send, recv, 0, {}

    def add(self, name, src, dst, device):
        i = self.count
        self.count += 1
        c = pltpu.make_async_remote_copy(
            src_ref=src,
            dst_ref=dst,
            send_sem=self.send.at[i],
            recv_sem=self.recv.at[i],
            device_id=device,
            device_id_type=MESH,
        )
        self.made[name] = c
        c.start()

    def got(self, name):
        self.made[name].wait_recv()

    def drain(self):
        for c in self.made.values():
            c.wait_send()


N_COPIES = 160


def kernel(
    tok_in, og_in, rwt, idx, gw_h, uw_h, dw_h,
    gg_h, ug_h, dg_h, rowdx, rowprob, picks,
    tk, gr, sc, tkt, gw, uw, dw, part, dbuf, fa, fb, rl, rr, hh, h0t, pcol,
    lgs, lgr, prs, prr, dps, dpr, dxs, dxr, dxo, wout,
    send_sem, recv_sem, wsem, osem,
):
    z = lax.axis_index("dp")
    y = lax.axis_index("expert")
    t = lax.axis_index("tensor")
    x = t // 2
    c = t % 2
    right, left = (x + 1) % 4, (x + 3) % 4
    across = (x + 2) % 4
    t_right, t_left, t_sib = right * 2 + c, left * 2 + c, x * 2 + (1 - c)

    wcopies = [
        pltpu.make_async_copy(a, b, wsem.at[i])
        for i, (a, b) in enumerate(((gw_h, gw), (uw_h, uw), (dw_h, dw)))
    ]
    for w in wcopies:
        w.start()

    barrier = pltpu.get_barrier_semaphore()
    for k in range(1, 8):
        pl.semaphore_signal(barrier, inc=1, device_id={"dp": (z + k) % 8}, device_id_type=MESH)
        pl.semaphore_signal(barrier, inc=1, device_id={"tensor": (t + k) % 8}, device_id_type=MESH)
    pl.semaphore_wait(barrier, 14)

    cp = Copies(send_sem, recv_sem)

    slot_at = lax.broadcasted_iota(jnp.int32, (CAP, 128), 0)
    lane_at = lax.broadcasted_iota(jnp.int32, (CAP, 128), 1)
    eye = (slot_at == lane_at).astype(F32)
    e0, e1, s0, s1 = idx[0:1, :], idx[1:2, :], idx[2:3, :], idx[3:4, :]
    table0 = jnp.where((e0 == y) & (s0 == slot_at), 1.0, 0.0).astype(F32)
    table1 = jnp.where((e1 == y) & (s1 == slot_at), 1.0, 0.0).astype(F32)
    select = (table0 + table1).astype(BF16)

    tk[0:CAP, :] = dot_nn(select, tok_in[...]).astype(BF16)
    gr[0:CAP, :] = dot_nn(select, og_in[...]).astype(BF16)

    def rows_of(p):
        return pl.ds(p * CAP, CAP)

    def ring(step, which):
        buf = tk if which == "t" else gr
        cp.add(("r", step + 1, which), buf.at[rows_of(place(-step))],
               buf.at[rows_of(place(-step - 1))], {"dp": (z + 1) % 8})

    def ring_back(step, which):
        buf = tk if which == "t" else gr
        cp.add(("l", step + 1, which), buf.at[rows_of(place(step))],
               buf.at[rows_of(place(step + 1))], {"dp": (z + 7) % 8})

    for which in "tg":
        ring(0, which)
        ring_back(0, which)

    lgs[...] = dot_nt(rwt[...], tok_in[...])
    for k in range(1, 8):
        cp.add(("lg", k), lgs, lgr.at[k], {"tensor": (t + k) % 8})

    def probabilities():
        total = lgs[...]
        for k in range(1, 8):
            cp.got(("lg", k))
            total = total + lgr[k]
        l0 = jnp.zeros((1, 128), F32)
        l1 = jnp.zeros((1, 128), F32)
        for j in range(4):
            l0 = l0 + jnp.where(e0 == j, total[j : j + 1, :], 0.0)
            l1 = l1 + jnp.where(e1 == j, total[j : j + 1, :], 0.0)
        p0 = jax.nn.sigmoid(l0 - l1)
        p1 = jax.nn.sigmoid(l1 - l0)
        picks[0:1, :] = p0
        picks[1:2, :] = p1
        low0 = p0.astype(BF16).astype(F32)
        low1 = p1.astype(BF16).astype(F32)
        col = jnp.sum(table0 * low0 + table1 * low1, axis=1, keepdims=True)
        pcol[0:CAP, :] = col
        prs[...] = jnp.broadcast_to(jnp.sum(eye * col, axis=0, keepdims=True), (8, 128))
        for k in range(1, 8):
            cp.add(("pr", k), prs, prr.at[place(-k)], {"dp": (z + k) % 8})

    def probability_of(p):
        o = ORDER[p]
        if o == 0:
            return
        cp.got(("pr", (-o) % 8))
        col = jnp.sum(eye * prr[p][0:1, :], axis=1, keepdims=True)
        pcol[p * CAP : (p + 1) * CAP, :] = col

    def arrive(p):
        o = ORDER[p]
        if o == 0:
            return
        if o == 4:
            cp.got(("r", 4, "t"))
            cp.got(("l", 4, "g"))
            return
        d = abs(o)
        for which in "tg":
            cp.got(("r" if o < 0 else "l", d, which))
            if o < 0:
                if d < 3 or which == "t":
                    ring(d, which)
            else:
                if d < 3 or which == "g":
                    ring_back(d, which)

    arrived = set()

    def arrive_all(ps):
        for p in ps:
            if p not in arrived:
                arrived.add(p)
                arrive(p)

    first = [True]

    def stage_f(k):
        p0, n = CHUNKS[k]
        r0, r = p0 * CAP, n * CAP
        for p in range(p0, p0 + n):
            if ORDER[p] == 4:
                arrive_all([POS[-3], POS[3]])
            arrive_all([p])
        if first[0]:
            for w in wcopies:
                w.wait()
            first[0] = False
        rows = pl.ds(r0, r)
        a = tk[r0 : r0 + r, :]
        b = gr[r0 : r0 + r, :]

        @pl.loop(0, 4)
        def _(n):
            cols = pl.ds(pl.multiple_of(n * 256, 256), 256)
            for m, v in enumerate((
                dot_nn(a, gw[:, cols]), dot_nn(a, uw[:, cols]), dot_nt(b, dw[cols, :]),
            )):
                v = v.astype(BF16)
                part[0, n, rows, m * 128 : m * 128 + 128] = v[:, 0:128]
                part[1, n, rows, m * 128 : m * 128 + 128] = v[:, 128:256]

        cp.add(("d2d", k), part.at[1 - c, :, rows, :], dbuf.at[:, rows, :], {"tensor": t_sib})

    def halves(k):
        p0, n = CHUNKS[k]
        r0, r = p0 * CAP, n * CAP
        h = r // 2
        return slice(r0, r0 + h), slice(r0 + h, r0 + r), pl.ds(r0, h), pl.ds(r0 + h, h)

    def fold(target, rows):
        v = part[c, target, rows, :].astype(F32) + dbuf[target, rows, :].astype(F32)
        part[c, target, rows, :] = v.astype(BF16)

    def stage_r1(k):
        sa, sb, da, db = halves(k)
        cp.got(("d2d", k))
        fold(across, sa)
        cp.add(("fa", k), part.at[c, across, da, :], fa.at[da, :], {"tensor": t_right})
        fold(across, sb)
        cp.add(("fb", k), part.at[c, across, db, :], fb.at[db, :], {"tensor": t_left})
        fold(right, sb)
        cp.add(("rlb", k), part.at[c, right, db, :], rl.at[db, :], {"tensor": t_right})
        fold(left, sa)
        cp.add(("rra", k), part.at[c, left, da, :], rr.at[da, :], {"tensor": t_left})

    def fold2(target, rows, extra):
        v = part[c, target, rows, :].astype(F32) + dbuf[target, rows, :].astype(F32)
        v = v + extra[rows, :].astype(F32)
        part[c, target, rows, :] = v.astype(BF16)

    def stage_r2(k):
        sa, sb, da, db = halves(k)
        cp.got(("fa", k))
        fold2(right, sa, fa)
        cp.add(("rla", k), part.at[c, right, da, :], rl.at[da, :], {"tensor": t_right})
        cp.got(("fb", k))
        fold2(left, sb, fb)
        cp.add(("rrb", k), part.at[c, left, db, :], rr.at[db, :], {"tensor": t_left})

    def tcols(q):
        return pl.ds(pl.multiple_of(q * 128, 128), 128)

    def h_copy(name, rows, q, device):
        ref = hh.at[:, rows, tcols(q)]
        cp.add(name, ref, ref, {"tensor": device})

    def stage_e(k):
        p0, n = CHUNKS[k]
        sa, sb, da, db = halves(k)
        for p in range(p0, p0 + n):
            probability_of(p)
        for s, names in ((sb, ("rlb", "rrb")), (sa, ("rla", "rra"))):
            for q in names:
                cp.got((q, k))
            v = part[c, x, s, :].astype(F32) + dbuf[x, s, :].astype(F32)
            v = v + rl[s, :].astype(F32) + rr[s, :].astype(F32)
            gate, up, ga = v[:, 0:128], v[:, 128:256], v[:, 256:384]
            g = jax.nn.sigmoid(gate)
            hid = (gate * g * up).astype(BF16)
            pcol_s = pcol[s, :]
            a = pcol_s * ga
            hh[0, s, tcols(t)] = hid
            hh[1, s, tcols(t)] = (a * up * g * (1.0 + gate * (1.0 - g))).astype(BF16)
            hh[2, s, tcols(t)] = (a * gate * g).astype(BF16)
            dpc = jnp.sum(hid.astype(F32) * ga, axis=1, keepdims=True)
            dprob_parts[(k, s.start)] = dpc
        h_copy(("ra", k), da, t, t_right)
        h_copy(("lb", k), db, t, t_left)
        h_copy(("rb", k), db, t, t_right)
        h_copy(("la", k), da, t, t_left)
        h_copy(("so", k), pl.ds(sa.start, 2 * (sa.stop - sa.start)), t, t_sib)
        dp_col = jnp.concatenate([dprob_parts[(k, sa.start)], dprob_parts[(k, sb.start)]], axis=0)
        for i in range(n):
            p = p0 + i
            row = jnp.sum(eye * dp_col[i * CAP : (i + 1) * CAP, :], axis=0, keepdims=True)
            dps[p] = jnp.broadcast_to(row, (8, 128))
            o = ORDER[p]
            if o != 0:
                cp.add(("dp", o), dps.at[p], dpr.at[place(-o)], {"dp": (z + o) % 8})
        for i in range(n):
            s = slice((p0 + i) * CAP, (p0 + i + 1) * CAP)
            sc[s, :] = (pcol[s, :] * gr[s, :].astype(F32)).astype(BF16)

    dprob_parts = {}

    def stage_g1(k):
        sa, sb, da, db = halves(k)
        full = pl.ds(sa.start, 2 * (sa.stop - sa.start))
        cp.got(("ra", k))
        h_copy(("xa", k), da, t_left, t_right)
        cp.got(("lb", k))
        h_copy(("xb", k), db, t_right, t_left)
        cp.got(("rb", k))
        h_copy(("sl", k), full, t_left, t_sib)
        cp.got(("la", k))
        h_copy(("sr", k), full, t_right, t_sib)

    def stage_g2(k):
        sa, sb, da, db = halves(k)
        full = pl.ds(sa.start, 2 * (sa.stop - sa.start))
        cp.got(("xa", k))
        cp.got(("xb", k))
        h_copy(("sx", k), full, across * 2 + c, t_sib)

    def stage_x(k):
        p0, n = CHUNKS[k]
        r0, r = p0 * CAP, n * CAP
        for q in ("so", "sl", "sr", "sx"):
            cp.got((q, k))
        a = hh[1, r0 : r0 + r, :]
        b = hh[2, r0 : r0 + r, :]

        @pl.loop(0, 3)
        def _(n):
            cols = pl.ds(pl.multiple_of(n * 256, 256), 256)
            v = dot_nt(a, gw[cols, :]) + dot_nt(b, uw[cols, :])
            if ORDER[p0] == 0:
                dxo[:, cols] = v[0:CAP]
            dxs[r0 : r0 + r, cols] = v.astype(BF16)

        for p in range(p0, p0 + n):
            o = ORDER[p]
            if o != 0:
                cp.add(("dx", o), dxs.at[rows_of(p)], dxr.at[rows_of(place(-o))],
                       {"dp": (z + o) % 8})

    run = {"F": stage_f, "R1": stage_r1, "R2": stage_r2, "E": stage_e,
           "G1": stage_g1, "G2": stage_g2, "X": stage_x}
    steps = plan()
    last_f = max(i for i, (s, _) in enumerate(steps) if s == "F")
    for i, (s, k) in enumerate(steps):
        if s == "R1" and k == 0:
            probabilities()
        run[s](k)
        if i == last_f:
            @pl.loop(0, 3)
            def _(n):
                cols = pl.ds(pl.multiple_of(n * 256, 256), 256)
                tkt[cols, :] = tk[:, cols].T

    @pl.loop(0, 4)
    def _(n):
        cols = pl.ds(pl.multiple_of(n * 256, 256), 256)
        h0t[cols, :] = hh[0, :, cols].T

    @pl.loop(0, 3)
    def _(i):
        rows = pl.ds(pl.multiple_of(i * 256, 256), 256)
        lhs = tkt[rows, :]

        @pl.loop(0, 4)
        def _(n):
            cols = pl.ds(pl.multiple_of(n * 256, 256), 256)
            wout[0, rows, cols] = dot_nn(lhs, hh[1, :, cols]).astype(BF16)
            wout[1, rows, cols] = dot_nn(lhs, hh[2, :, cols]).astype(BF16)

    outs = [pltpu.make_async_copy(wout.at[0], gg_h, osem.at[0]),
            pltpu.make_async_copy(wout.at[1], ug_h, osem.at[1]),
            pltpu.make_async_copy(dw, dg_h, osem.at[2])]
    outs[0].start()
    outs[1].start()

    @pl.loop(0, 4)
    def _(i):
        rows = pl.ds(pl.multiple_of(i * 256, 256), 256)
        lhs = h0t[rows, :]

        @pl.loop(0, 3)
        def _(n):
            cols = pl.ds(pl.multiple_of(n * 256, 256), 256)
            dw[rows, cols] = dot_nn(lhs, sc[:, cols]).astype(BF16)

    outs[2].start()

    total = dxo[...]
    prob = dps[0]
    for p in range(8):
        o = ORDER[p]
        if o != 0:
            cp.got(("dp", -o if o != 4 else 4))
            prob = prob + dpr[p]
            cp.got(("dx", -o if o != 4 else 4))
            total = total + dxr[p * CAP : (p + 1) * CAP, :].astype(F32)
    rowdx[...] = total
    rowprob[...] = prob
    for o in outs:
        o.wait()
    cp.drain()


def mega(tokens, out_grad, rwt, idx, gate_w, up_w, down_w):
    vm = pl.BlockSpec(memory_space=pltpu.VMEM)
    hbm = pl.BlockSpec(memory_space=pl.ANY)
    V = pltpu.VMEM
    return pl.pallas_call(
        kernel,
        name="moe_backward",
        in_specs=[vm] * 4 + [hbm] * 3,
        out_specs=[hbm] * 3 + [vm] * 3,
        out_shape=[
            jax.ShapeDtypeStruct((768, 1024), BF16),
            jax.ShapeDtypeStruct((768, 1024), BF16),
            jax.ShapeDtypeStruct((1024, 768), BF16),
            jax.ShapeDtypeStruct((CAP, 768), F32),
            jax.ShapeDtypeStruct((8, 128), F32),
            jax.ShapeDtypeStruct((2, 128), F32),
        ],
        scratch_shapes=[
            V((768, 768), BF16), V((768, 768), BF16), V((768, 768), BF16), V((768, 768), BF16),
            V((768, 1024), BF16), V((768, 1024), BF16), V((1024, 768), BF16),
            V((2, 4, 768, 384), BF16), V((4, 768, 384), BF16),
            V((768, 384), BF16), V((768, 384), BF16), V((768, 384), BF16), V((768, 384), BF16),
            V((3, 768, 1024), BF16), V((1024, 768), BF16), V((768, 1), F32),
            V((8, 128), F32), V((8, 8, 128), F32), V((8, 128), F32), V((8, 8, 128), F32),
            V((8, 8, 128), F32), V((8, 8, 128), F32),
            V((768, 768), BF16), V((768, 768), BF16), V((CAP, 768), F32),
            V((2, 768, 1024), BF16),
            pltpu.SemaphoreType.DMA((N_COPIES,)), pltpu.SemaphoreType.DMA((N_COPIES,)),
            pltpu.SemaphoreType.DMA((3,)), pltpu.SemaphoreType.DMA((3,)),
        ],
        compiler_params=pltpu.CompilerParams(
            collective_id=0, has_side_effects=True, vmem_limit_bytes=56 * 1024 * 1024
        ),
    )(tokens, out_grad, rwt, idx, gate_w, up_w, down_w)


def from_everyone(array, axis):
    count = lax.axis_size(axis)
    return lax.all_to_all(
        jnp.broadcast_to(array[None], (count, *array.shape)), axis, 0, 0, tiled=True
    )


def of_everyone(array, axis):
    return from_everyone(array, axis).sum(axis=0)


def split_up(array, dim, count):
    before, after = (array.shape[:dim], array.shape[dim + 1 :])
    return jnp.moveaxis(array.reshape(*before, count, -1, *after), dim, 0)


def sent_and_summed(array, axis, dim):
    parts = split_up(array, dim, lax.axis_size(axis))
    arrived = lax.all_to_all(parts, axis, split_axis=0, concat_axis=0, tiled=True)
    return arrived.astype(jnp.float32).sum(axis=0)


def in_one_piece_2(arrays, axis, dim, along):
    both = jnp.concatenate(arrays, axis=along)
    filled, at, gathered = (sent_and_summed(both, axis, dim), 0, [])
    for a in arrays:
        gathered.append(lax.slice_in_dim(filled, at, at + a.shape[along], axis=along))
        at += a.shape[along]
    return tuple(gathered)


def split_parts(values):
    high_part = values.astype(jnp.bfloat16)
    low_part = (values - high_part.astype(jnp.float32)).astype(jnp.bfloat16)
    return (high_part, low_part)


def table_apply(form, table_low, values):
    high_part, low_part = split_parts(values)
    return jnp.einsum(form, table_low, high_part, preferred_element_type=jnp.float32) + jnp.einsum(
        form, table_low, low_part, preferred_element_type=jnp.float32
    )


def slot_table(experts_here, slots_here, expert_id, capacity):
    positions = lax.broadcasted_iota(jnp.int32, (capacity, experts_here.shape[0]), 0)
    first_table = (experts_here[:, 0] == expert_id)[None, :] & (
        slots_here[:, 0][None, :] == positions
    )
    second_table = (experts_here[:, 1] == expert_id)[None, :] & (
        slots_here[:, 1][None, :] == positions
    )
    return (first_table.astype(jnp.float32), second_table.astype(jnp.float32))


def shards(
    tokens, out_grad, router_weight, gate_weight, up_weight, down_weight, expert_index, slot_index
):
    expert_count = router_weight.shape[1]
    expert_id = lax.axis_index("expert")
    rwt = jnp.concatenate([router_weight.T, jnp.zeros((4, router_weight.shape[0]), BF16)], axis=0)
    idx = jnp.concatenate([expert_index, slot_index], axis=1).T
    gate_grad, up_grad, down_grad, row_dx, prob8, picks = mega(
        tokens, out_grad, rwt, idx, gate_weight[0], up_weight[0], down_weight[0]
    )
    row_prob = prob8[0, :CAP]
    pick_prob = picks.T
    first_table, second_table = slot_table(expert_index, slot_index, expert_id, CAP)
    select_low = (first_table + second_table).astype(jnp.bfloat16)
    own_expert = (lax.broadcasted_iota(jnp.int32, (1, expert_count), 1) == expert_id).astype(
        jnp.float32
    )
    token_dx = table_apply("cn,cd->nd", select_low, row_dx)
    token_prob = table_apply("cn,c->n", select_low, row_prob)
    token_term, prob_rows = in_one_piece_2(
        (token_dx.astype(jnp.bfloat16), (token_prob[:, None] * own_expert).astype(jnp.bfloat16)),
        "expert",
        0,
        1,
    )
    prob_rows = of_everyone(prob_rows, "tensor")
    quarter = token_term.shape[0]
    offset = expert_id * quarter
    part_prob = lax.dynamic_slice_in_dim(pick_prob, offset, quarter, 0)
    part_experts = lax.dynamic_slice_in_dim(expert_index, offset, quarter, 0)
    part_tokens = lax.dynamic_slice_in_dim(tokens, offset, quarter, 0)
    pick_grad = jnp.take_along_axis(prob_rows, part_experts, axis=1)
    mixed_grad = jnp.sum(part_prob * pick_grad, axis=1, keepdims=True)
    weights = part_prob * (pick_grad - mixed_grad)
    onehot = (
        part_experts[:, :, None] == lax.broadcasted_iota(jnp.int32, (1, 1, expert_count), 2)
    ).astype(jnp.float32)
    logit_grad = jnp.sum(onehot * weights[:, :, None], axis=1)
    router_rows = router_weight.astype(jnp.float32)
    tokens_grad = (token_term + jnp.dot(logit_grad, router_rows.T)).astype(jnp.bfloat16)
    router_part = jnp.dot(part_tokens.astype(jnp.float32).T, logit_grad)
    router_grad = of_everyone(router_part, ("dp", "expert"))
    return (tokens_grad, router_grad, gate_grad[None], up_grad[None], down_grad[None])


def solution(mesh):
    in_specs = (
        P("dp", "tensor"),
        P("dp", "tensor"),
        P("tensor", None),
        P("expert", "tensor", "dp"),
        P("expert", "tensor", "dp"),
        P("expert", "dp", "tensor"),
        P("dp", None),
        P("dp", None),
    )
    out_specs = (
        P(("dp", "expert"), "tensor"),
        P("tensor", None),
        P("expert", "tensor", "dp"),
        P("expert", "tensor", "dp"),
        P("expert", "dp", "tensor"),
    )
    return jax.shard_map(shards, mesh=mesh, in_specs=in_specs, out_specs=out_specs, check_vma=False)
```

```python
import jax
import jax.numpy as jnp
from jax import lax
from jax.experimental import pallas as pl
from jax.experimental.pallas import tpu as pltpu
from jax.sharding import PartitionSpec as P

CAP = 96
MESH = pl.DeviceIdType.MESH
F32 = jnp.float32
BF16 = jnp.bfloat16

ORDER = (0, -1, 1, -2, 2, 4, -3, 3)
GROUPS = (1, 2, 2, 1, 2)
POS = {o: i for i, o in enumerate(ORDER)}


def place(offset):
    o = offset % 8
    return POS[o if o <= 4 else o - 8]


CHUNKS = []
_at = 0
for _n in GROUPS:
    CHUNKS.append((_at, _n))
    _at += _n

STAGES = ("F", "R1", "R2", "E", "G1", "G2", "X")
SKEW = 1


def plan():
    steps = []
    last = len(STAGES) + SKEW * (len(CHUNKS) - 1)
    for s in range(last):
        for k in range(len(CHUNKS)):
            i = s - SKEW * k
            if 0 <= i < len(STAGES):
                steps.append((STAGES[i], k))
    return steps


def dot_nt(a, b):
    return lax.dot_general(a, b, (((1,), (1,)), ((), ())), preferred_element_type=F32)


def dot_nn(a, b):
    return lax.dot_general(a, b, (((1,), (0,)), ((), ())), preferred_element_type=F32)


class Copies:
    def __init__(self, send, recv):
        self.send, self.recv, self.count, self.made = send, recv, 0, {}

    def add(self, name, src, dst, device):
        i = self.count
        self.count += 1
        c = pltpu.make_async_remote_copy(
            src_ref=src,
            dst_ref=dst,
            send_sem=self.send.at[i],
            recv_sem=self.recv.at[i],
            device_id=device,
            device_id_type=MESH,
        )
        self.made[name] = c
        c.start()

    def got(self, name):
        self.made[name].wait_recv()

    def drain(self):
        for c in self.made.values():
            c.wait_send()


N_COPIES = 160


def kernel(
    tok_in, og_in, rwt, ex, sl, gw_h, uw_h, dw_h,
    tok_out, router_out, gg_h, ug_h, dg_h,
    tk, gr, sc, tkt, gw, uw, dw, part, dbuf, fa, fb, rl, rr, hh, h0t, pcol,
    lgs, lgr, prs, prr, dps, dpr, dxs, dxr, dxo, wout,
    pts, ptr, pys, pyr, ws, wr, rgs, rgr, yd, yr, lg3,
    send_sem, recv_sem, wsem, osem,
):
    z = lax.axis_index("dp")
    y = lax.axis_index("expert")
    t = lax.axis_index("tensor")
    x = t // 2
    c = t % 2
    right, left = (x + 1) % 4, (x + 3) % 4
    across = (x + 2) % 4
    t_right, t_left, t_sib = right * 2 + c, left * 2 + c, x * 2 + (1 - c)

    wcopies = [
        pltpu.make_async_copy(a, b, wsem.at[i])
        for i, (a, b) in enumerate(((gw_h, gw), (uw_h, uw), (dw_h, dw)))
    ]
    for w in wcopies:
        w.start()

    barrier = pltpu.get_barrier_semaphore()
    for k in range(1, 8):
        pl.semaphore_signal(barrier, inc=1, device_id={"dp": (z + k) % 8}, device_id_type=MESH)
        pl.semaphore_signal(barrier, inc=1, device_id={"tensor": (t + k) % 8}, device_id_type=MESH)
    for k in range(1, 4):
        pl.semaphore_signal(barrier, inc=1, device_id={"expert": (y + k) % 4}, device_id_type=MESH)
    pl.semaphore_wait(barrier, 17)

    cp = Copies(send_sem, recv_sem)

    slot_at = lax.broadcasted_iota(jnp.int32, (CAP, 128), 0)
    lane_at = lax.broadcasted_iota(jnp.int32, (CAP, 128), 1)
    eye = (slot_at == lane_at).astype(F32)
    e0, e1, s0, s1 = ex[0:1, :], ex[1:2, :], sl[0:1, :], sl[1:2, :]
    table0 = jnp.where((e0 == y) & (s0 == slot_at), 1.0, 0.0).astype(F32)
    table1 = jnp.where((e1 == y) & (s1 == slot_at), 1.0, 0.0).astype(F32)
    select = (table0 + table1).astype(BF16)

    tk[0:CAP, :] = dot_nn(select, tok_in[...]).astype(BF16)
    gr[0:CAP, :] = dot_nn(select, og_in[...]).astype(BF16)

    def rows_of(p):
        return pl.ds(p * CAP, CAP)

    def ring(step, which):
        buf = tk if which == "t" else gr
        cp.add(("r", step + 1, which), buf.at[rows_of(place(-step))],
               buf.at[rows_of(place(-step - 1))], {"dp": (z + 1) % 8})

    def ring_back(step, which):
        buf = tk if which == "t" else gr
        cp.add(("l", step + 1, which), buf.at[rows_of(place(step))],
               buf.at[rows_of(place(step + 1))], {"dp": (z + 7) % 8})

    for which in "tg":
        ring(0, which)
        ring_back(0, which)

    lgs[4:8, :] = jnp.zeros((4, 128), F32)
    lgs[0:4, :] = dot_nt(rwt[...], tok_in[...])
    for k in range(1, 8):
        cp.add(("lg", k), lgs, lgr.at[k], {"tensor": (t + k) % 8})

    picks = []

    def probabilities():
        total = lgs[0:4, :]
        for k in range(1, 8):
            cp.got(("lg", k))
            total = total + lgr[k][0:4, :]
        l0 = jnp.zeros((1, 128), F32)
        l1 = jnp.zeros((1, 128), F32)
        for j in range(4):
            l0 = l0 + jnp.where(e0 == j, total[j : j + 1, :], 0.0)
            l1 = l1 + jnp.where(e1 == j, total[j : j + 1, :], 0.0)
        p0 = jax.nn.sigmoid(l0 - l1)
        p1 = jax.nn.sigmoid(l1 - l0)
        picks.extend((p0, p1))
        low0 = p0.astype(BF16).astype(F32)
        low1 = p1.astype(BF16).astype(F32)
        col = jnp.sum(table0 * low0 + table1 * low1, axis=1, keepdims=True)
        pcol[0:CAP, :] = col
        prs[...] = jnp.broadcast_to(jnp.sum(eye * col, axis=0, keepdims=True), (8, 128))
        for k in range(1, 8):
            cp.add(("pr", k), prs, prr.at[place(-k)], {"dp": (z + k) % 8})

    def probability_of(p):
        o = ORDER[p]
        if o == 0:
            return
        cp.got(("pr", (-o) % 8))
        col = jnp.sum(eye * prr[p][0:1, :], axis=1, keepdims=True)
        pcol[p * CAP : (p + 1) * CAP, :] = col

    def arrive(p):
        o = ORDER[p]
        if o == 0:
            return
        if o == 4:
            cp.got(("r", 4, "t"))
            cp.got(("l", 4, "g"))
            return
        d = abs(o)
        for which in "tg":
            cp.got(("r" if o < 0 else "l", d, which))
            if o < 0:
                if d < 3 or which == "t":
                    ring(d, which)
            else:
                if d < 3 or which == "g":
                    ring_back(d, which)

    arrived = set()

    def arrive_all(ps):
        for p in ps:
            if p not in arrived:
                arrived.add(p)
                arrive(p)

    first = [True]

    def stage_f(k):
        p0, n = CHUNKS[k]
        r0, r = p0 * CAP, n * CAP
        for p in range(p0, p0 + n):
            if ORDER[p] == 4:
                arrive_all([POS[-3], POS[3]])
            arrive_all([p])
        if first[0]:
            for w in wcopies:
                w.wait()
            first[0] = False
        rows = pl.ds(r0, r)
        a = tk[r0 : r0 + r, :]
        b = gr[r0 : r0 + r, :]

        @pl.loop(0, 4)
        def _(n):
            cols = pl.ds(pl.multiple_of(n * 256, 256), 256)
            for m, v in enumerate((
                dot_nn(a, gw[:, cols]), dot_nn(a, uw[:, cols]), dot_nt(b, dw[cols, :]),
            )):
                v = v.astype(BF16)
                part[0, n, rows, m * 128 : m * 128 + 128] = v[:, 0:128]
                part[1, n, rows, m * 128 : m * 128 + 128] = v[:, 128:256]

        cp.add(("d2d", k), part.at[1 - c, :, rows, :], dbuf.at[:, rows, :], {"tensor": t_sib})

    def halves(k):
        p0, n = CHUNKS[k]
        r0, r = p0 * CAP, n * CAP
        h = r // 2
        return slice(r0, r0 + h), slice(r0 + h, r0 + r), pl.ds(r0, h), pl.ds(r0 + h, h)

    def fold(target, rows):
        v = part[c, target, rows, :].astype(F32) + dbuf[target, rows, :].astype(F32)
        part[c, target, rows, :] = v.astype(BF16)

    def stage_r1(k):
        sa, sb, da, db = halves(k)
        cp.got(("d2d", k))
        fold(across, sa)
        cp.add(("fa", k), part.at[c, across, da, :], fa.at[da, :], {"tensor": t_right})
        fold(across, sb)
        cp.add(("fb", k), part.at[c, across, db, :], fb.at[db, :], {"tensor": t_left})
        fold(right, sb)
        cp.add(("rlb", k), part.at[c, right, db, :], rl.at[db, :], {"tensor": t_right})
        fold(left, sa)
        cp.add(("rra", k), part.at[c, left, da, :], rr.at[da, :], {"tensor": t_left})

    def fold2(target, rows, extra):
        v = part[c, target, rows, :].astype(F32) + dbuf[target, rows, :].astype(F32)
        v = v + extra[rows, :].astype(F32)
        part[c, target, rows, :] = v.astype(BF16)

    def stage_r2(k):
        sa, sb, da, db = halves(k)
        cp.got(("fa", k))
        fold2(right, sa, fa)
        cp.add(("rla", k), part.at[c, right, da, :], rl.at[da, :], {"tensor": t_right})
        cp.got(("fb", k))
        fold2(left, sb, fb)
        cp.add(("rrb", k), part.at[c, left, db, :], rr.at[db, :], {"tensor": t_left})

    def tcols(q):
        return pl.ds(pl.multiple_of(q * 128, 128), 128)

    def h_copy(name, rows, q, device):
        ref = hh.at[:, rows, tcols(q)]
        cp.add(name, ref, ref, {"tensor": device})

    def stage_e(k):
        p0, n = CHUNKS[k]
        sa, sb, da, db = halves(k)
        for p in range(p0, p0 + n):
            probability_of(p)
        for s, names in ((sb, ("rlb", "rrb")), (sa, ("rla", "rra"))):
            for q in names:
                cp.got((q, k))
            v = part[c, x, s, :].astype(F32) + dbuf[x, s, :].astype(F32)
            v = v + rl[s, :].astype(F32) + rr[s, :].astype(F32)
            gate, up, ga = v[:, 0:128], v[:, 128:256], v[:, 256:384]
            g = jax.nn.sigmoid(gate)
            hid = (gate * g * up).astype(BF16)
            pcol_s = pcol[s, :]
            a = pcol_s * ga
            hh[0, s, tcols(t)] = hid
            hh[1, s, tcols(t)] = (a * up * g * (1.0 + gate * (1.0 - g))).astype(BF16)
            hh[2, s, tcols(t)] = (a * gate * g).astype(BF16)
            dpc = jnp.sum(hid.astype(F32) * ga, axis=1, keepdims=True)
            dprob_parts[(k, s.start)] = dpc
        h_copy(("ra", k), da, t, t_right)
        h_copy(("lb", k), db, t, t_left)
        h_copy(("rb", k), db, t, t_right)
        h_copy(("la", k), da, t, t_left)
        h_copy(("so", k), pl.ds(sa.start, 2 * (sa.stop - sa.start)), t, t_sib)
        dp_col = jnp.concatenate([dprob_parts[(k, sa.start)], dprob_parts[(k, sb.start)]], axis=0)
        for i in range(n):
            p = p0 + i
            row = jnp.sum(eye * dp_col[i * CAP : (i + 1) * CAP, :], axis=0, keepdims=True)
            dps[p] = jnp.broadcast_to(row, (8, 128))
            o = ORDER[p]
            if o != 0:
                cp.add(("dp", o), dps.at[p], dpr.at[place(-o)], {"dp": (z + o) % 8})
        for i in range(n):
            s = slice((p0 + i) * CAP, (p0 + i + 1) * CAP)
            sc[s, :] = (pcol[s, :] * gr[s, :].astype(F32)).astype(BF16)

    dprob_parts = {}

    def stage_g1(k):
        sa, sb, da, db = halves(k)
        full = pl.ds(sa.start, 2 * (sa.stop - sa.start))
        cp.got(("ra", k))
        h_copy(("xa", k), da, t_left, t_right)
        cp.got(("lb", k))
        h_copy(("xb", k), db, t_right, t_left)
        cp.got(("rb", k))
        h_copy(("sl", k), full, t_left, t_sib)
        cp.got(("la", k))
        h_copy(("sr", k), full, t_right, t_sib)

    def stage_g2(k):
        sa, sb, da, db = halves(k)
        full = pl.ds(sa.start, 2 * (sa.stop - sa.start))
        cp.got(("xa", k))
        cp.got(("xb", k))
        h_copy(("sx", k), full, across * 2 + c, t_sib)

    def stage_x(k):
        p0, n = CHUNKS[k]
        r0, r = p0 * CAP, n * CAP
        for q in ("so", "sl", "sr", "sx"):
            cp.got((q, k))
        a = hh[1, r0 : r0 + r, :]
        b = hh[2, r0 : r0 + r, :]

        @pl.loop(0, 3)
        def _(n):
            cols = pl.ds(pl.multiple_of(n * 256, 256), 256)
            v = dot_nt(a, gw[cols, :]) + dot_nt(b, uw[cols, :])
            if ORDER[p0] == 0:
                dxo[:, cols] = v[0:CAP]
            dxs[r0 : r0 + r, cols] = v.astype(BF16)

        for p in range(p0, p0 + n):
            o = ORDER[p]
            if o != 0:
                cp.add(("dx", o), dxs.at[rows_of(p)], dxr.at[rows_of(place(-o))],
                       {"dp": (z + o) % 8})

    def to_col(row):
        return jnp.sum(eye * row, axis=1, keepdims=True)

    def to_row(col):
        return jnp.sum(eye * col, axis=0, keepdims=True)

    def parts3(v):
        hi = v.astype(BF16)
        rest = v - hi.astype(F32)
        mid = rest.astype(BF16)
        low = (rest - mid.astype(F32)).astype(BF16)
        return hi, mid, low

    def pair8(r0, r1):
        row = lax.broadcasted_iota(jnp.int32, (8, 128), 0)
        return jnp.where(row == 0, r0, jnp.where(row == 1, r1, 0.0))

    def router_1():
        total = dps[0][0:1, :]
        for p in range(8):
            if ORDER[p] != 0:
                o = ORDER[p]
                cp.got(("dp", -o if o != 4 else 4))
                total = total + dpr[p][0:1, :]
        col = to_col(total)
        pts[...] = pair8(jnp.sum(table0 * col, axis=0, keepdims=True),
                         jnp.sum(table1 * col, axis=0, keepdims=True))
        for k in range(1, 8):
            cp.add(("pt", k), pts, ptr.at[k], {"tensor": (t + k) % 8})

    def router_2():
        total = pts[...]
        for k in range(1, 8):
            cp.got(("pt", k))
            total = total + ptr[k]
        pys[...] = total
        for k in range(1, 4):
            cp.add(("py", k), pys, pyr.at[k], {"expert": (y + k) % 4})

    def router_3():
        total = pys[...]
        for k in range(1, 4):
            cp.got(("py", k))
            total = total + pyr[k]
        d0, d1 = total[0:1, :], total[1:2, :]
        p0, p1 = picks
        mixed = p0 * d0 + p1 * d1
        w0 = p0 * (d0 - mixed)
        w1 = p1 * (d1 - mixed)
        ws[...] = jnp.broadcast_to(
            to_row(jnp.sum(table0 * w0 + table1 * w1, axis=1, keepdims=True)), (8, 128))
        for k in range(1, 8):
            cp.add(("w", k), ws, wr.at[place(-k)], {"dp": (z + k) % 8})
        i0 = lax.broadcasted_iota(jnp.int32, (128, 128), 0)
        i1 = lax.broadcasted_iota(jnp.int32, (128, 128), 1)
        eye_t = (i0 == i1).astype(F32)

        def col_t(row):
            return jnp.sum(eye_t * row, axis=1, keepdims=True)

        lane = lax.broadcasted_iota(jnp.int32, (128, 16), 1)
        of_expert = (lane % 4).astype(F32)
        v = (jnp.where(col_t(e0.astype(F32)) == of_expert, col_t(w0), 0.0)
             + jnp.where(col_t(e1.astype(F32)) == of_expert, col_t(w1), 0.0))
        hi, mid, low = (q.astype(F32) for q in parts3(v))
        lg3[...] = jnp.where(lane < 4, hi, jnp.where(lane < 8, mid, jnp.where(lane < 12, low, 0.0)))

    def router_4():
        acc = jnp.zeros((8, 768), F32)
        row = lax.broadcasted_iota(jnp.int32, (8, 128), 0)
        for p in range(8):
            if ORDER[p] == 0:
                v = ws[...]
            else:
                cp.got(("w", (-ORDER[p]) % 8))
                v = wr[p]
            hi, mid, low = (q.astype(F32) for q in parts3(v))
            lhs = jnp.where(row == 0, hi, jnp.where(row == 1, mid, jnp.where(row == 2, low, 0.0)))
            acc = acc + dot_nn(lhs[:, 0:CAP].astype(BF16), tk[p * CAP : (p + 1) * CAP, :])
        rgs[...] = jnp.broadcast_to(jnp.sum(acc, axis=0, keepdims=True), (8, 768))
        rgr[0] = rgs[...]
        for k in range(1, 4):
            cp.add(("rg", k), rgs, rgr.at[k], {"expert": (y + k) % 4})

    def router_5():
        for k in range(1, 4):
            cp.got(("rg", k))
        for j in range(4):
            k = (y + 4 - j) % 4
            router_out[j : j + 1, :] = rgr[k][0:1, :]

    def tokens_1():
        total = dxo[...]
        for p in range(8):
            o = ORDER[p]
            if o != 0:
                cp.got(("dx", -o if o != 4 else 4))
                total = total + dxr[p * CAP : (p + 1) * CAP, :].astype(F32)
        hi = total.astype(BF16)
        low = (total - hi.astype(F32)).astype(BF16)
        both = jnp.concatenate([hi, low], axis=0)
        pick = jnp.concatenate([select.astype(F32).T.astype(BF16)] * 2, axis=1)
        v = dot_nn(pick, both)
        yd[...] = v.astype(BF16)
        for k in range(1, 4):
            rows = pl.ds(pl.multiple_of(((y + k) % 4) * 32, 32), 32)
            cp.add(("yd", k), yd.at[rows, :], yr.at[k], {"expert": (y + k) % 4})

    def tokens_2():
        rows = pl.ds(pl.multiple_of(y * 32, 32), 32)
        total = yd[rows, :].astype(F32)
        total = total + dot_nn(lg3[rows, :].astype(BF16), jnp.concatenate([rwt[...]] * 4, axis=0))
        for k in range(1, 4):
            cp.got(("yd", k))
            total = total + yr[k].astype(F32)
        tok_out[...] = total.astype(BF16)

    def fill_1():
        @pl.loop(0, 3)
        def _(n):
            cols = pl.ds(pl.multiple_of(n * 256, 256), 256)
            tkt[cols, :] = tk[:, cols].T

    outs = [pltpu.make_async_copy(wout.at[0], gg_h, osem.at[0]),
            pltpu.make_async_copy(wout.at[1], ug_h, osem.at[1]),
            pltpu.make_async_copy(dw, dg_h, osem.at[2])]

    def weights_1():
        @pl.loop(0, 3)
        def _(i):
            rows = pl.ds(pl.multiple_of(i * 256, 256), 256)
            lhs = tkt[rows, :]

            @pl.loop(0, 4)
            def _(n):
                cols = pl.ds(pl.multiple_of(n * 256, 256), 256)
                wout[0, rows, cols] = dot_nn(lhs, hh[1, :, cols]).astype(BF16)
                wout[1, rows, cols] = dot_nn(lhs, hh[2, :, cols]).astype(BF16)

        outs[0].start()
        outs[1].start()

    def weights_2():
        @pl.loop(0, 4)
        def _(i):
            rows = pl.ds(pl.multiple_of(i * 256, 256), 256)
            h0t[...] = hh[0, :, rows].T

            @pl.loop(0, 3)
            def _(n):
                cols = pl.ds(pl.multiple_of(n * 256, 256), 256)
                dw[rows, cols] = dot_nn(h0t[...], sc[:, cols]).astype(BF16)

        outs[2].start()

    run = {"F": stage_f, "R1": stage_r1, "R2": stage_r2, "E": stage_e,
           "G1": stage_g1, "G2": stage_g2, "X": stage_x}
    steps = plan()
    end = len(CHUNKS) - 1
    last_f = max(i for i, (s, _) in enumerate(steps) if s == "F")
    for i, (s, k) in enumerate(steps):
        if s == "R1" and k == 0:
            probabilities()
        run[s](k)
        if i == last_f:
            fill_1()
        if (s, k) == ("G1", end):
            router_1()
        if (s, k) == ("G2", end):
            router_2()
    router_3()
    weights_1()
    router_4()
    tokens_1()
    weights_2()
    router_5()
    tokens_2()
    for o in outs:
        o.wait()
    cp.drain()


def shards(
    tokens, out_grad, router_weight, gate_weight, up_weight, down_weight, expert_index, slot_index
):
    vm = pl.BlockSpec(memory_space=pltpu.VMEM)
    hbm = pl.BlockSpec(memory_space=pl.ANY)
    V = pltpu.VMEM
    small = V((8, 128), F32)
    several = V((8, 8, 128), F32)
    tokens_grad, router_grad, gate_grad, up_grad, down_grad = pl.pallas_call(
        kernel,
        name="moe_backward",
        in_specs=[vm] * 5 + [hbm] * 3,
        out_specs=[vm] * 2 + [hbm] * 3,
        out_shape=[
            jax.ShapeDtypeStruct((32, 768), BF16),
            jax.ShapeDtypeStruct((4, 768), F32),
            jax.ShapeDtypeStruct((768, 1024), BF16),
            jax.ShapeDtypeStruct((768, 1024), BF16),
            jax.ShapeDtypeStruct((1024, 768), BF16),
        ],
        scratch_shapes=[
            V((768, 768), BF16), V((768, 768), BF16), V((768, 768), BF16), V((768, 768), BF16),
            V((768, 1024), BF16), V((768, 1024), BF16), V((1024, 768), BF16),
            V((2, 4, 768, 384), BF16), V((4, 768, 384), BF16),
            V((768, 384), BF16), V((768, 384), BF16), V((768, 384), BF16), V((768, 384), BF16),
            V((3, 768, 1024), BF16), V((256, 768), BF16), V((768, 1), F32),
            small, several, small, several, several, several,
            V((768, 768), BF16), V((768, 768), BF16), V((CAP, 768), F32),
            V((2, 768, 1024), BF16),
            small, several, small, V((4, 8, 128), F32), small, several,
            V((8, 768), F32), V((4, 8, 768), F32), V((128, 768), BF16), V((4, 32, 768), BF16),
            V((128, 16), F32),
            pltpu.SemaphoreType.DMA((N_COPIES,)), pltpu.SemaphoreType.DMA((N_COPIES,)),
            pltpu.SemaphoreType.DMA((3,)), pltpu.SemaphoreType.DMA((3,)),
        ],
        compiler_params=pltpu.CompilerParams(
            collective_id=0, has_side_effects=True, vmem_limit_bytes=56 * 1024 * 1024
        ),
    )(
        tokens, out_grad, router_weight.T, expert_index.T, slot_index.T,
        gate_weight[0], up_weight[0], down_weight[0],
    )
    return (tokens_grad, router_grad.T, gate_grad[None], up_grad[None], down_grad[None])


def solution(mesh):
    in_specs = (
        P("dp", "tensor"),
        P("dp", "tensor"),
        P("tensor", None),
        P("expert", "tensor", "dp"),
        P("expert", "tensor", "dp"),
        P("expert", "dp", "tensor"),
        P("dp", None),
        P("dp", None),
    )
    out_specs = (
        P(("dp", "expert"), "tensor"),
        P("tensor", None),
        P("expert", "tensor", "dp"),
        P("expert", "tensor", "dp"),
        P("expert", "dp", "tensor"),
    )
    return jax.shard_map(shards, mesh=mesh, in_specs=in_specs, out_specs=out_specs, check_vma=False)
```

```python
import jax
import jax.numpy as jnp
from jax import lax
from jax.experimental import pallas as pl
from jax.experimental.pallas import tpu as pltpu
from jax.sharding import PartitionSpec as P

CAP = 96
MESH = pl.DeviceIdType.MESH
F32 = jnp.float32
BF16 = jnp.bfloat16

ORDER = (0, -1, 1, -2, 2, -3, 3, 4)
GROUPS = (1, 2, 2, 2, 1)
POS = {o: i for i, o in enumerate(ORDER)}


def place(offset):
    o = offset % 8
    return POS[o if o <= 4 else o - 8]


CHUNKS = []
_at = 0
for _n in GROUPS:
    CHUNKS.append((_at, _n))
    _at += _n

STEPS = (
    ("F", 0, 2), ("F", 0, 1), ("F", 0, 3), ("F", 0, 0), ("open",), ("D", 0, 2), ("D", 0, 1),
    ("D", 0, 3), ("D", 0, 0), ("R1", 0, 2), ("R1", 0, 1), ("R1", 0, 3), ("prob",), ("R2", 0, 0),
    ("R2", 0, 1), ("Z", 1, "t"), ("Z", 1, "g"), ("F", 1, 2), ("D", 1, 2), ("E", 0), ("F", 1, 1),
    ("D", 1, 1), ("F", 1, 3), ("D", 1, 3), ("F", 1, 0), ("D", 1, 0), ("R1", 1, 2), ("Z", 2, "t"),
    ("G", 0, 0), ("G", 0, 1), ("R1", 1, 1), ("G", 0, 2), ("G", 0, 3), ("R1", 1, 3), ("R2", 1, 0),
    ("R2", 1, 1), ("Z", 2, "g"), ("F", 2, 2), ("D", 2, 2), ("G", 0, 4), ("F", 2, 1), ("D", 2, 1),
    ("F", 2, 3), ("D", 2, 3), ("F", 2, 0), ("D", 2, 0), ("R1", 2, 2), ("X", 0), ("Z", 3, "t"),
    ("E", 1), ("R1", 2, 1), ("R1", 2, 3), ("R2", 2, 0), ("R2", 2, 1), ("Z", 3, "g"), ("F", 3, 2),
    ("D", 3, 2), ("F", 3, 1), ("D", 3, 1), ("F", 3, 3), ("D", 3, 3), ("F", 3, 0), ("D", 3, 0),
    ("G", 1, 0), ("G", 1, 1), ("R1", 3, 2), ("R1", 3, 1), ("G", 1, 2), ("G", 1, 3), ("Y", 0),
    ("R1", 3, 3), ("F", 4, 2), ("D", 4, 2), ("F", 4, 1), ("D", 4, 1), ("F", 4, 3), ("D", 4, 3),
    ("F", 4, 0), ("D", 4, 0), ("E", 2), ("R1", 4, 2), ("T",), ("R1", 4, 1), ("R1", 4, 3),
    ("G", 1, 4), ("R2", 3, 0), ("R2", 3, 1), ("X", 1), ("G", 2, 0), ("G", 2, 1), ("G", 2, 2),
    ("G", 2, 3), ("R2", 4, 0), ("R2", 4, 1), ("E", 3), ("G", 2, 4), ("E", 4), ("Y", 1), ("X", 2),
    ("G", 3, 0), ("G", 3, 1), ("G", 3, 2), ("G", 3, 3), ("G", 4, 0), ("G", 4, 1), ("P1",),
    ("G", 4, 2), ("G", 4, 3), ("G", 3, 4), ("G", 4, 4), ("P2",), ("X", 3), ("X", 4), ("P3",),
    ("Y", 2), ("W1", 0), ("W1", 1), ("W1", 2), ("P4",), ("W2", 0), ("W2", 1), ("Y", 3), ("W2", 2),
    ("W2", 3), ("P5",), ("Y", 4), ("end",),
)


def dot_nt(a, b):
    return lax.dot_general(a, b, (((1,), (1,)), ((), ())), preferred_element_type=F32)


def dot_nn(a, b):
    return lax.dot_general(a, b, (((1,), (0,)), ((), ())), preferred_element_type=F32)


class Copies:
    def __init__(self, send, recv):
        self.send, self.recv, self.count, self.made = send, recv, 0, {}

    def add(self, name, src, dst, device):
        i = self.count
        self.count += 1
        c = pltpu.make_async_remote_copy(
            src_ref=src,
            dst_ref=dst,
            send_sem=self.send.at[i],
            recv_sem=self.recv.at[i],
            device_id=device,
            device_id_type=MESH,
        )
        self.made[name] = c
        c.start()

    def got(self, name):
        self.made[name].wait_recv()

    def drain(self):
        for c in self.made.values():
            c.wait_send()


N_COPIES = 220


def kernel(
    tok_h, og_h, rwt_h, ex_h, sl_h, gw_h, uw_h, dw_h,
    tok_out, router_out, gg_o, ug_o, dg_o,
    tk, gr, sc, tkt, gw, uw, dw, part, dbuf, fa, fb, rl, rr, hh, h0t, pcol,
    lgs, lgr, prs, prr, dps, dpr, ix, yd, yr, yq, zq, own_q,
    pts, ptr, pys, pyr, ws, wr, rgs, rgr, lg3,
    tok_in, og_in, rwt, ex, sl, send_sem, recv_sem, wsem,
):
    z = lax.axis_index("dp")
    y = lax.axis_index("expert")
    t = lax.axis_index("tensor")
    x = t // 2
    c = t % 2
    right, left, across = (x + 1) % 4, (x + 3) % 4, (x + 2) % 4
    turn = (x, right, across, left)
    t_right, t_left, t_sib = right * 2 + c, left * 2 + c, x * 2 + (1 - c)

    loads = [
        pltpu.make_async_copy(a, b, wsem.at[i])
        for i, (a, b) in enumerate((
            (ex_h, ex), (sl_h, sl), (tok_h, tok_in), (og_h, og_in), (rwt_h, rwt),
            (gw_h, gw), (uw_h, uw), (dw_h, dw),
        ))
    ]
    for w in loads:
        w.start()
    wcopies = loads[5:]

    barrier = pltpu.get_barrier_semaphore()
    for k in range(1, 8):
        pl.semaphore_signal(barrier, inc=1, device_id={"dp": (z + k) % 8}, device_id_type=MESH)
        pl.semaphore_signal(barrier, inc=1, device_id={"tensor": (t + k) % 8}, device_id_type=MESH)
    for k in range(1, 4):
        pl.semaphore_signal(barrier, inc=1, device_id={"expert": (y + k) % 4}, device_id_type=MESH)

    cp = Copies(send_sem, recv_sem)

    for w in loads[:5]:
        w.wait()

    slot_at = lax.broadcasted_iota(jnp.int32, (CAP, 128), 0)
    lane_at = lax.broadcasted_iota(jnp.int32, (CAP, 128), 1)
    eye = (slot_at == lane_at).astype(F32)
    e0, e1, s0, s1 = ex[0:1, :], ex[1:2, :], sl[0:1, :], sl[1:2, :]

    def table(e, s):
        return jnp.where((e == y) & (s == slot_at), 1.0, 0.0).astype(F32)

    table0, table1 = table(e0, s0), table(e1, s1)
    select = (table0 + table1).astype(BF16)
    tk[0:CAP, :] = dot_nn(select, tok_in[...]).astype(BF16)
    gr[0:CAP, :] = dot_nn(select, og_in[...]).astype(BF16)
    lgs[4:8, :] = jnp.zeros((4, 128), F32)
    lgs[0:4, :] = dot_nt(rwt[...], tok_in[...])
    ix[0] = jnp.zeros((8, 128), jnp.int32)
    ix[0, 0:2, :] = ex[...]
    ix[0, 2:4, :] = sl[...]

    def rows_of(p):
        return pl.ds(p * CAP, CAP)

    def ring(step, which):
        buf = tk if which == "t" else gr
        cp.add(("r", step + 1, which), buf.at[rows_of(place(-step))],
               buf.at[rows_of(place(-step - 1))], {"dp": (z + 1) % 8})

    def ring_back(step, which):
        buf = tk if which == "t" else gr
        cp.add(("l", step + 1, which), buf.at[rows_of(place(step))],
               buf.at[rows_of(place(step + 1))], {"dp": (z + 7) % 8})

    def to_col(row):
        return jnp.sum(eye * row, axis=1, keepdims=True)

    def to_row(col):
        return jnp.sum(eye * col, axis=0, keepdims=True)

    def parts3(v):
        hi = v.astype(BF16)
        rest = v - hi.astype(F32)
        mid = rest.astype(BF16)
        low = (rest - mid.astype(F32)).astype(BF16)
        return hi, mid, low

    def rows8(*given):
        row = lax.broadcasted_iota(jnp.int32, (8, 128), 0)
        v = jnp.zeros((8, 128), F32)
        for i, r in enumerate(given):
            v = jnp.where(row == i, r, v)
        return v

    picks = []

    def open_up():
        pl.semaphore_wait(barrier, 17)
        for which in "tg":
            ring(0, which)
            ring_back(0, which)
        for k in range(1, 8):
            cp.add(("lg", k), lgs, lgr.at[k], {"tensor": (t + k) % 8})
        for k in range(1, 8):
            cp.add(("ix", k), ix.at[0], ix.at[place(-k)], {"dp": (z + k) % 8})

    def probabilities():
        total = lgs[0:4, :]
        for k in range(1, 8):
            cp.got(("lg", k))
            total = total + lgr[k][0:4, :]
        l0 = jnp.zeros((1, 128), F32)
        l1 = jnp.zeros((1, 128), F32)
        for j in range(4):
            l0 = l0 + jnp.where(e0 == j, total[j : j + 1, :], 0.0)
            l1 = l1 + jnp.where(e1 == j, total[j : j + 1, :], 0.0)
        p0 = jax.nn.sigmoid(l0 - l1)
        p1 = jax.nn.sigmoid(l1 - l0)
        picks.extend((p0, p1))
        low0 = p0.astype(BF16).astype(F32)
        low1 = p1.astype(BF16).astype(F32)
        col = jnp.sum(table0 * low0 + table1 * low1, axis=1, keepdims=True)
        pcol[0:CAP, :] = col
        prs[...] = jnp.broadcast_to(to_row(col), (8, 128))
        for k in range(1, 8):
            cp.add(("pr", k), prs, prr.at[place(-k)], {"dp": (z + k) % 8})

    def pass_on(d, which):
        cp.got(("r", d, which))
        if d < 3 or which == "t":
            ring(d, which)
        cp.got(("l", d, which))
        if d < 3 or which == "g":
            ring_back(d, which)

    def rows_in(k):
        p0, n = CHUNKS[k]
        return p0 * CAP, n * CAP

    def halves(k):
        r0, r = rows_in(k)
        h = r // 2
        return slice(r0, r0 + h), slice(r0 + h, r0 + r), pl.ds(r0, h), pl.ds(r0 + h, h)

    ready = []

    def forward(k, j):
        p0, n = CHUNKS[k]
        r0, r = rows_in(k)
        if not ready:
            for w in wcopies:
                w.wait()
            ready.append(1)
        if j == 2 and 4 in ORDER[p0 : p0 + n]:
            cp.got(("r", 4, "t"))
            cp.got(("l", 4, "g"))
        a = tk[r0 : r0 + r, :]
        b = gr[r0 : r0 + r, :]
        q = turn[j]
        cols = pl.ds(pl.multiple_of(q * 256, 256), 256)
        for m, v in enumerate((
            dot_nn(a, gw[:, cols]), dot_nn(a, uw[:, cols]), dot_nt(b, dw[cols, :]),
        )):
            v = v.astype(BF16)
            part[0, q, r0 : r0 + r, m * 128 : m * 128 + 128] = v[:, 0:128]
            part[1, q, r0 : r0 + r, m * 128 : m * 128 + 128] = v[:, 128:256]

    def to_sibling(k, j):
        r0, r = rows_in(k)
        rows = pl.ds(r0, r)
        q = turn[j]
        cp.add(("d", k, j), part.at[1 - c, q, rows, :], dbuf.at[q, rows, :], {"tensor": t_sib})

    def fold(target, rows, extra=None):
        v = part[c, target, rows, :].astype(F32) + dbuf[target, rows, :].astype(F32)
        if extra is not None:
            v = v + extra[rows, :].astype(F32)
        part[c, target, rows, :] = v.astype(BF16)

    def reduce_1(k, j):
        sa, sb, da, db = halves(k)
        cp.got(("d", k, j))
        if j == 2:
            fold(across, sa)
            cp.add(("fa", k), part.at[c, across, da, :], fa.at[da, :], {"tensor": t_right})
            fold(across, sb)
            cp.add(("fb", k), part.at[c, across, db, :], fb.at[db, :], {"tensor": t_left})
        if j == 1:
            fold(right, sb)
            cp.add(("rlb", k), part.at[c, right, db, :], rl.at[db, :], {"tensor": t_right})
        if j == 3:
            fold(left, sa)
            cp.add(("rra", k), part.at[c, left, da, :], rr.at[da, :], {"tensor": t_left})

    def reduce_2(k, side):
        sa, sb, da, db = halves(k)
        if side == 0:
            cp.got(("fa", k))
            fold(right, sa, fa)
            cp.add(("rla", k), part.at[c, right, da, :], rl.at[da, :], {"tensor": t_right})
        else:
            cp.got(("fb", k))
            fold(left, sb, fb)
            cp.add(("rrb", k), part.at[c, left, db, :], rr.at[db, :], {"tensor": t_left})

    def tcols(q):
        return pl.ds(pl.multiple_of(q * 128, 128), 128)

    def h_copy(name, rows, q, device):
        ref = hh.at[:, rows, tcols(q)]
        cp.add(name, ref, ref, {"tensor": device})

    def activate(k):
        p0, n = CHUNKS[k]
        sa, sb, da, db = halves(k)
        for p in range(p0, p0 + n):
            if ORDER[p] != 0:
                cp.got(("pr", (-ORDER[p]) % 8))
                pcol[p * CAP : (p + 1) * CAP, :] = to_col(prr[p][0:1, :])
        cp.got(("d", k, 0))
        sums = []
        for s, names in ((sb, ("rlb", "rrb")), (sa, ("rla", "rra"))):
            for q in names:
                cp.got((q, k))
            v = part[c, x, s, :].astype(F32) + dbuf[x, s, :].astype(F32)
            v = v + rl[s, :].astype(F32) + rr[s, :].astype(F32)
            gate, up, ga = v[:, 0:128], v[:, 128:256], v[:, 256:384]
            g = jax.nn.sigmoid(gate)
            hid = (gate * g * up).astype(BF16)
            a = pcol[s, :] * ga
            hh[0, s, tcols(t)] = hid
            hh[1, s, tcols(t)] = (a * up * g * (1.0 + gate * (1.0 - g))).astype(BF16)
            hh[2, s, tcols(t)] = (a * gate * g).astype(BF16)
            sums.insert(0, jnp.sum(hid.astype(F32) * ga, axis=1, keepdims=True))
        h_copy(("ra", k), da, t, t_right)
        h_copy(("lb", k), db, t, t_left)
        h_copy(("rb", k), db, t, t_right)
        h_copy(("la", k), da, t, t_left)
        h_copy(("so", k), pl.ds(*rows_in(k)), t, t_sib)
        col = jnp.concatenate(sums, axis=0)
        for i in range(n):
            p = p0 + i
            dps[p] = jnp.broadcast_to(to_row(col[i * CAP : (i + 1) * CAP, :]), (8, 128))
            o = ORDER[p]
            if o != 0:
                cp.add(("dp", o), dps.at[p], dpr.at[place(-o)], {"dp": (z + o) % 8})
        for p in range(p0, p0 + n):
            s = slice(p * CAP, (p + 1) * CAP)
            sc[s, :] = (pcol[s, :] * gr[s, :].astype(F32)).astype(BF16)

    def spread(k, i):
        sa, sb, da, db = halves(k)
        full = pl.ds(*rows_in(k))
        if i == 0:
            cp.got(("ra", k))
            h_copy(("xa", k), da, t_left, t_right)
        if i == 1:
            cp.got(("lb", k))
            h_copy(("xb", k), db, t_right, t_left)
        if i == 2:
            cp.got(("rb", k))
            h_copy(("sl", k), full, t_left, t_sib)
        if i == 3:
            cp.got(("la", k))
            h_copy(("sr", k), full, t_right, t_sib)
        if i == 4:
            cp.got(("xa", k))
            cp.got(("xb", k))
            h_copy(("sx", k), full, across * 2 + c, t_sib)

    def backward(k):
        p0, n = CHUNKS[k]
        r0, r = rows_in(k)
        for q in ("so", "sl", "sr", "sx"):
            cp.got((q, k))
        a = hh[1, r0 : r0 + r, :]
        b = hh[2, r0 : r0 + r, :]
        turned = []
        for p in range(p0, p0 + n):
            if ORDER[p] != 0:
                cp.got(("ix", (-ORDER[p]) % 8))
            v = ix[p]
            both = table(v[0:1, :], v[2:3, :]) + table(v[1:2, :], v[3:4, :])
            turned.append(both.T.astype(BF16))
        for m in range(3):
            cols = slice(m * 256, m * 256 + 256)
            v = (dot_nt(a, gw[cols, :]) + dot_nt(b, uw[cols, :])).astype(BF16)
            for i in range(n):
                yd[p0 + i, :, cols] = dot_nn(
                    turned[i], v[i * CAP : (i + 1) * CAP, :]).astype(BF16)
        for q in range(1, 4):
            rows = pl.ds(pl.multiple_of(((y + q) % 4) * 32, 32), 32)
            cp.add(("y", k, q), yd.at[pl.ds(p0, n), rows, :], yr.at[q, pl.ds(p0, n)],
                   {"expert": (y + q) % 4})

    def homeward(k):
        p0, n = CHUNKS[k]
        for q in range(1, 4):
            cp.got(("y", k, q))
        rows = pl.ds(pl.multiple_of(y * 32, 32), 32)
        for p in range(p0, p0 + n):
            v = yd[p, rows, :].astype(F32)
            for q in range(1, 4):
                v = v + yr[q, p].astype(F32)
            o = ORDER[p]
            if o == 0:
                own_q[...] = v
            else:
                yq[p] = v.astype(BF16)
                cp.add(("z", o), yq.at[p], zq.at[place(-o)], {"dp": (z + o) % 8})

    def router_1():
        total = dps[0][0:1, :]
        for p in range(8):
            if ORDER[p] != 0:
                o = ORDER[p]
                cp.got(("dp", -o if o != 4 else 4))
                total = total + dpr[p][0:1, :]
        col = to_col(total)
        pts[...] = rows8(jnp.sum(table0 * col, axis=0, keepdims=True),
                         jnp.sum(table1 * col, axis=0, keepdims=True))
        for k in range(1, 8):
            cp.add(("pt", k), pts, ptr.at[k], {"tensor": (t + k) % 8})

    def router_2():
        total = pts[...]
        for k in range(1, 8):
            cp.got(("pt", k))
            total = total + ptr[k]
        pys[...] = total
        for k in range(1, 4):
            cp.add(("py", k), pys, pyr.at[k], {"expert": (y + k) % 4})

    def router_3():
        total = pys[...]
        for k in range(1, 4):
            cp.got(("py", k))
            total = total + pyr[k]
        d0, d1 = total[0:1, :], total[1:2, :]
        p0, p1 = picks
        mixed = p0 * d0 + p1 * d1
        w0 = p0 * (d0 - mixed)
        w1 = p1 * (d1 - mixed)
        ws[...] = jnp.broadcast_to(
            to_row(jnp.sum(table0 * w0 + table1 * w1, axis=1, keepdims=True)), (8, 128))
        for k in range(1, 8):
            cp.add(("w", k), ws, wr.at[place(-k)], {"dp": (z + k) % 8})
        i0 = lax.broadcasted_iota(jnp.int32, (128, 128), 0)
        i1 = lax.broadcasted_iota(jnp.int32, (128, 128), 1)
        eye_t = (i0 == i1).astype(F32)

        def col_t(row):
            return jnp.sum(eye_t * row, axis=1, keepdims=True)

        lane = lax.broadcasted_iota(jnp.int32, (128, 16), 1)
        of_expert = (lane % 4).astype(F32)
        v = (jnp.where(col_t(e0.astype(F32)) == of_expert, col_t(w0), 0.0)
             + jnp.where(col_t(e1.astype(F32)) == of_expert, col_t(w1), 0.0))
        hi, mid, low = (q.astype(F32) for q in parts3(v))
        lg3[...] = jnp.where(lane < 4, hi, jnp.where(lane < 8, mid, jnp.where(lane < 12, low, 0.0)))

    def router_4():
        acc = jnp.zeros((8, 768), F32)
        for p in range(8):
            if ORDER[p] == 0:
                v = ws[0:1, :]
            else:
                cp.got(("w", (-ORDER[p]) % 8))
                v = wr[p][0:1, :]
            lhs = rows8(*(q.astype(F32) for q in parts3(v)))
            acc = acc + dot_nn(lhs[:, 0:CAP].astype(BF16), tk[p * CAP : (p + 1) * CAP, :])
        rgs[...] = jnp.broadcast_to(jnp.sum(acc, axis=0, keepdims=True), (8, 768))
        rgr[0] = rgs[...]
        for k in range(1, 4):
            cp.add(("rg", k), rgs, rgr.at[k], {"expert": (y + k) % 4})

    def router_5():
        for k in range(1, 4):
            cp.got(("rg", k))
        for j in range(4):
            k = (y + 4 - j) % 4
            router_out[j : j + 1, :] = rgr[k][0:1, :]

    def finish():
        rows = pl.ds(pl.multiple_of(y * 32, 32), 32)
        total = own_q[...]
        total = total + dot_nn(lg3[rows, :].astype(BF16), jnp.concatenate([rwt[...]] * 4, axis=0))
        for p in range(8):
            o = ORDER[p]
            if o != 0:
                cp.got(("z", -o if o != 4 else 4))
                total = total + zq[p].astype(F32)
        tok_out[...] = total.astype(BF16)

    def turn_tokens():
        @pl.loop(0, 3)
        def _(n):
            cols = pl.ds(pl.multiple_of(n * 256, 256), 256)
            tkt[cols, :] = tk[:, cols].T

    def weights_1(i):
        rows = slice(i * 256, i * 256 + 256)
        lhs = tkt[rows, :]

        @pl.loop(0, 4)
        def _(n):
            cols = pl.ds(pl.multiple_of(n * 256, 256), 256)
            gg_o[rows, cols] = dot_nn(lhs, hh[1, :, cols]).astype(BF16)
            ug_o[rows, cols] = dot_nn(lhs, hh[2, :, cols]).astype(BF16)

    def weights_2(i):
        rows = slice(i * 256, i * 256 + 256)
        h0t[...] = hh[0, :, rows].T

        @pl.loop(0, 3)
        def _(n):
            cols = pl.ds(pl.multiple_of(n * 256, 256), 256)
            dg_o[rows, cols] = dot_nn(h0t[...], sc[:, cols]).astype(BF16)

    run = {
        "open": open_up, "prob": probabilities, "Z": pass_on, "F": forward, "D": to_sibling,
        "R1": reduce_1, "R2": reduce_2, "E": activate, "G": spread, "X": backward,
        "Y": homeward, "P1": router_1, "P2": router_2, "P3": router_3, "P4": router_4,
        "P5": router_5, "T": turn_tokens, "W1": weights_1, "W2": weights_2, "end": finish,
    }
    for step in STEPS:
        run[step[0]](*step[1:])
    cp.drain()


def put_out(*refs):
    sem = refs[10]
    copies = [pltpu.make_async_copy(refs[i], refs[5 + i], sem.at[i]) for i in range(5)]
    for q in copies:
        q.start()
    for q in copies:
        q.wait()


def shards(
    tokens, out_grad, router_weight, gate_weight, up_weight, down_weight, expert_index, slot_index
):
    vm = pl.BlockSpec(memory_space=pltpu.VMEM)
    hbm = pl.BlockSpec(memory_space=pltpu.HBM)
    V = pltpu.VMEM
    small = V((8, 128), F32)
    several = V((8, 8, 128), F32)
    out_shape = [
        jax.ShapeDtypeStruct((32, 768), BF16),
        jax.ShapeDtypeStruct((4, 768), F32),
        jax.ShapeDtypeStruct((768, 1024), BF16),
        jax.ShapeDtypeStruct((768, 1024), BF16),
        jax.ShapeDtypeStruct((1024, 768), BF16),
    ]
    results = pl.pallas_call(
        kernel,
        name="moe_backward",
        in_specs=[hbm] * 8,
        out_specs=[vm] * 5,
        out_shape=out_shape,
        scratch_shapes=[
            V((768, 768), BF16), V((768, 768), BF16), V((768, 768), BF16), V((768, 768), BF16),
            V((768, 1024), BF16), V((768, 1024), BF16), V((1024, 768), BF16),
            V((2, 4, 768, 384), BF16), V((4, 768, 384), BF16),
            V((768, 384), BF16), V((768, 384), BF16), V((768, 384), BF16), V((768, 384), BF16),
            V((3, 768, 1024), BF16), V((256, 768), BF16), V((768, 1), F32),
            small, several, small, several, several, several, V((8, 8, 128), jnp.int32),
            V((8, 128, 768), BF16), V((4, 8, 32, 768), BF16), V((8, 32, 768), BF16),
            V((8, 32, 768), BF16), V((32, 768), F32),
            small, several, small, V((4, 8, 128), F32), small, several,
            V((8, 768), F32), V((4, 8, 768), F32), V((128, 16), F32),
            V((128, 768), BF16), V((128, 768), BF16), V((4, 768), BF16),
            V((2, 128), jnp.int32), V((2, 128), jnp.int32),
            pltpu.SemaphoreType.DMA((N_COPIES,)), pltpu.SemaphoreType.DMA((N_COPIES,)),
            pltpu.SemaphoreType.DMA((8,)),
        ],
        compiler_params=pltpu.CompilerParams(
            collective_id=0, has_side_effects=True, vmem_limit_bytes=40 * 1024 * 1024
        ),
    )(
        *(pltpu.with_memory_space_constraint(v, pltpu.HBM) for v in (
            tokens, out_grad, router_weight.T, expert_index.T, slot_index.T,
            gate_weight[0], up_weight[0], down_weight[0],
        ))
    )
    tokens_grad, router_grad, gate_grad, up_grad, down_grad = pl.pallas_call(
        put_out,
        name="put_out",
        in_specs=[vm] * 5,
        out_specs=[hbm] * 5,
        out_shape=out_shape,
        scratch_shapes=[pltpu.SemaphoreType.DMA((5,))],
        compiler_params=pltpu.CompilerParams(vmem_limit_bytes=1024 * 1024),
    )(*results)
    return (tokens_grad, router_grad.T, gate_grad[None], up_grad[None], down_grad[None])


def solution(mesh):
    in_specs = (
        P("dp", "tensor"),
        P("dp", "tensor"),
        P("tensor", None),
        P("expert", "tensor", "dp"),
        P("expert", "tensor", "dp"),
        P("expert", "dp", "tensor"),
        P("dp", None),
        P("dp", None),
    )
    out_specs = (
        P(("dp", "expert"), "tensor"),
        P("tensor", None),
        P("expert", "tensor", "dp"),
        P("expert", "tensor", "dp"),
        P("expert", "dp", "tensor"),
    )
    return jax.shard_map(shards, mesh=mesh, in_specs=in_specs, out_specs=out_specs, check_vma=False)
```

```python
import jax
import jax.numpy as jnp
from jax import lax
from jax.experimental import pallas as pl
from jax.experimental.pallas import tpu as pltpu
from jax.sharding import PartitionSpec as P

CAP = 96
MESH = pl.DeviceIdType.MESH
F32 = jnp.float32
BF16 = jnp.bfloat16

UNITS = ((0, 0), (0, 1), (-1, 0), (1, 0), (-1, 1), (1, 1), (-2, 0), (2, 0), (-2, 1), (2, 1), (4, 0), (4, 1), (-3, 0), (-3, 1), (3, 0), (3, 1))
GROUPS = (2, 2, 2, 2, 2, 2, 2, 2)
BACK = (1, 2, 2, 1, 1, 1)
HALF = CAP // 2
BLOCKS = (0, -1, 1, -2, 2, -3, 3, 4)
POS = {o: i for i, o in enumerate(BLOCKS)}
ROW = {u: i * HALF for i, u in enumerate(UNITS)}


def near(offset):
    o = offset % 8
    return o if o <= 4 else o - 8


def place(offset):
    return POS[near(offset)]


def runs(sizes):
    ends = [sum(sizes[: i + 1]) for i in range(len(sizes))]
    return [(e - n, n) for e, n in zip(ends, sizes)]


CHUNKS = runs(GROUPS)
BACKS = runs(BACK)

STEPS = (
    ("open",), ("F", 0, 2), ("D", 0, 2), ("F", 0, 1), ("D", 0, 1), ("F", 0, 3), ("D", 0, 3),
    ("F", 0, 0), ("D", 0, 0), ("S", 0), ("R1", 0, 2), ("R1", 0, 1), ("R1", 0, 3), ("R2", 0, 0),
    ("R2", 0, 1), ("Z", 1, 0), ("prob",), ("far", 2), ("F", 1, 2), ("D", 1, 2), ("F", 1, 1),
    ("D", 1, 1), ("F", 1, 3), ("D", 1, 3), ("F", 1, 0), ("D", 1, 0), ("R1", 1, 2), ("R1", 1, 1),
    ("E", 0), ("R1", 1, 3), ("Z", 1, 1), ("F", 2, 2), ("D", 2, 2), ("F", 2, 1), ("D", 2, 1),
    ("F", 2, 3), ("D", 2, 3), ("F", 2, 0), ("D", 2, 0), ("S", 1), ("S", 2), ("R1", 2, 2),
    ("R2", 1, 0), ("R2", 1, 1), ("R1", 2, 1), ("R1", 2, 3), ("G", 0, 1), ("Z", 2, 0), ("far", 3),
    ("F", 3, 2), ("D", 3, 2), ("G", 0, 0), ("G", 0, 3), ("F", 3, 1), ("D", 3, 1), ("F", 3, 3),
    ("D", 3, 3), ("G", 0, 2), ("F", 3, 0), ("D", 3, 0), ("R1", 3, 2), ("R2", 2, 0), ("R2", 2, 1),
    ("R1", 3, 1), ("E", 1), ("Z", 2, 1), ("R1", 3, 3), ("F", 4, 2), ("D", 4, 2), ("F", 4, 1),
    ("D", 4, 1), ("F", 4, 3), ("D", 4, 3), ("G", 0, 4), ("F", 4, 0), ("D", 4, 0), ("S", 3),
    ("S", 4), ("R1", 4, 2), ("R2", 3, 0), ("R2", 3, 1), ("R1", 4, 1), ("R1", 4, 3), ("E", 2),
    ("Z", 3, 0), ("far", 4), ("G", 1, 1), ("X", 0), ("G", 1, 0), ("G", 1, 3), ("G", 1, 2),
    ("R2", 4, 0), ("R2", 4, 1), ("Z", 3, 1), ("E", 3), ("G", 2, 0), ("G", 2, 1), ("V", 0),
    ("G", 2, 2), ("G", 2, 3), ("G", 1, 4), ("E", 4), ("G", 3, 0), ("G", 3, 1), ("F", 5, 2),
    ("D", 5, 2), ("Y", 0), ("G", 3, 2), ("G", 3, 3), ("F", 5, 1), ("D", 5, 1), ("F", 5, 3),
    ("D", 5, 3), ("G", 2, 4), ("F", 5, 0), ("D", 5, 0), ("R1", 5, 2), ("F", 6, 2), ("D", 6, 2),
    ("F", 6, 1), ("D", 6, 1), ("G", 4, 0), ("G", 4, 1), ("F", 6, 3), ("D", 6, 3), ("R1", 5, 1),
    ("F", 6, 0), ("D", 6, 0), ("G", 4, 2), ("G", 4, 3), ("R1", 5, 3), ("F", 7, 2), ("D", 7, 2),
    ("G", 3, 4), ("R1", 6, 2), ("R1", 6, 1), ("R2", 5, 0), ("R2", 5, 1), ("R1", 6, 3), ("X", 1),
    ("G", 4, 4), ("R1", 7, 2), ("F", 7, 1), ("D", 7, 1), ("F", 7, 3), ("D", 7, 3), ("R2", 6, 0),
    ("R2", 6, 1), ("F", 7, 0), ("D", 7, 0), ("S", 5), ("R1", 7, 1), ("R1", 7, 3), ("E", 5),
    ("R2", 7, 0), ("R2", 7, 1), ("X", 2), ("E", 6), ("V", 1), ("S", 6), ("S", 7), ("G", 5, 0),
    ("G", 5, 1), ("G", 5, 2), ("G", 5, 3), ("E", 7), ("G", 6, 0), ("G", 6, 1), ("V", 2),
    ("G", 6, 2), ("G", 6, 3), ("G", 5, 4), ("Y", 1), ("G", 7, 0), ("G", 7, 1), ("X", 3),
    ("G", 7, 2), ("G", 6, 4), ("G", 7, 3), ("Y", 2), ("P1",), ("G", 7, 4), ("X", 4), ("V", 3),
    ("X", 5), ("W", 0, 0), ("P3",), ("W", 0, 1), ("V", 4), ("W", 0, 2), ("W", 1, 0), ("Y", 3),
    ("W", 1, 1), ("V", 5), ("W", 1, 2), ("W", 2, 0), ("W", 2, 1), ("Y", 4), ("W", 2, 2),
    ("W", 2, 3), ("Y", 5), ("P5",), ("end",),
)


def dot_nt(a, b):
    return lax.dot_general(a, b, (((1,), (1,)), ((), ())), preferred_element_type=F32)


def dot_nn(a, b):
    return lax.dot_general(a, b, (((1,), (0,)), ((), ())), preferred_element_type=F32)


class Copies:
    def __init__(self, send, recv):
        self.send, self.recv, self.count, self.made = send, recv, 0, {}

    def add(self, name, src, dst, device):
        i = self.count
        self.count += 1
        c = pltpu.make_async_remote_copy(
            src_ref=src,
            dst_ref=dst,
            send_sem=self.send.at[i],
            recv_sem=self.recv.at[i],
            device_id=device,
            device_id_type=MESH,
        )
        self.made[name] = c
        c.start()

    def got(self, name):
        self.made[name].wait_recv()

    def drain(self):
        for c in self.made.values():
            c.wait_send()


N_COPIES = 340


def kernel(
    tok_h, og_h, rwt_h, ex_h, sl_h, gw_h, uw_h, dw_h,
    tok_out, router_out, gg_o, ug_o, dg_o,
    tk, gr, sc, gw, uw, dw, part, dbuf, fa, fb, rl, rr, hh, pcol, dcol,
    lgs, lgr, prs, prr, dps, dpr, ix, selt, dxs, yq, zq, own_q,
    pts, ptr, rgs, rgr, lg3,
    tok_in, og_in, rwt, ex, sl, send_sem, recv_sem, wsem, *sums,
):
    yd, ya, yb, yr, yl = (sums[i * len(BACKS) : (i + 1) * len(BACKS)] for i in range(5))
    z = lax.axis_index("dp")
    y = lax.axis_index("expert")
    t = lax.axis_index("tensor")
    x = t // 2
    c = t % 2
    right, left, across = (x + 1) % 4, (x + 3) % 4, (x + 2) % 4
    turn = (x, right, across, left)
    t_right, t_left, t_sib = right * 2 + c, left * 2 + c, x * 2 + (1 - c)

    loads = [
        pltpu.make_async_copy(a, b, wsem.at[i])
        for i, (a, b) in enumerate((
            (ex_h, ex), (sl_h, sl), (tok_h, tok_in), (og_h, og_in), (rwt_h, rwt),
            (gw_h, gw), (uw_h, uw), (dw_h, dw),
        ))
    ]
    for w in loads:
        w.start()
    wcopies = loads[5:]

    barrier = pltpu.get_barrier_semaphore()
    for k in (1, 7):
        pl.semaphore_signal(barrier, inc=1, device_id={"dp": (z + k) % 8}, device_id_type=MESH)
    for k in range(1, 32):
        pl.semaphore_signal(
            barrier, inc=1, device_id={"expert": (y + k // 8) % 4, "tensor": (t + k) % 8},
            device_id_type=MESH)

    cp = Copies(send_sem, recv_sem)

    for w in loads[:5]:
        w.wait()

    slot_at = lax.broadcasted_iota(jnp.int32, (CAP, 128), 0)
    lane_at = lax.broadcasted_iota(jnp.int32, (CAP, 128), 1)
    eye = (slot_at == lane_at).astype(F32)
    e0, e1, s0, s1 = ex[0:1, :], ex[1:2, :], sl[0:1, :], sl[1:2, :]

    def table(e, s):
        return jnp.where((e == y) & (s == slot_at), 1.0, 0.0).astype(F32)

    table0, table1 = table(e0, s0), table(e1, s1)
    select = (table0 + table1).astype(BF16)
    tk[0:CAP, :] = dot_nn(select, tok_in[...]).astype(BF16)
    gr[0:CAP, :] = dot_nn(select, og_in[...]).astype(BF16)
    lgs[4:8, :] = jnp.zeros((4, 128), F32)
    lgs[0:4, :] = dot_nt(rwt[...], tok_in[...])
    ix[0] = jnp.zeros((8, 128), jnp.int32)
    ix[0, 0:2, :] = ex[...]
    ix[0, 2:4, :] = sl[...]

    def ring(step, half):
        for which, buf in (("t", tk), ("g", gr)):
            cp.add(("r", step + 1, half, which), buf.at[pl.ds(ROW[near(-step), half], HALF)],
                   buf.at[pl.ds(ROW[near(-step - 1), half], HALF)], {"dp": (z + 1) % 8})

    def ring_back(step, half):
        for which, buf in (("t", tk), ("g", gr)):
            cp.add(("l", step + 1, half, which), buf.at[pl.ds(ROW[near(step), half], HALF)],
                   buf.at[pl.ds(ROW[near(step + 1), half], HALF)], {"dp": (z + 7) % 8})

    def to_col(row):
        return jnp.sum(eye * row, axis=1, keepdims=True)

    def to_row(col):
        return jnp.sum(eye * col, axis=0, keepdims=True)

    def parts3(v):
        hi = v.astype(BF16)
        rest = v - hi.astype(F32)
        mid = rest.astype(BF16)
        low = (rest - mid.astype(F32)).astype(BF16)
        return hi, mid, low

    def rows8(*given):
        row = lax.broadcasted_iota(jnp.int32, (8, 128), 0)
        v = jnp.zeros((8, 128), F32)
        for i, r in enumerate(given):
            v = jnp.where(row == i, r, v)
        return v

    picks = []

    def open_up():
        pl.semaphore_wait(barrier, 33)
        for k in (1, 7):
            cp.add(("ix", k), ix.at[0], ix.at[place(-k)], {"dp": (z + k) % 8})
        for half in range(2):
            ring(0, half)
            ring_back(0, half)
        for k in range(1, 8):
            cp.add(("lg", k), lgs, lgr.at[k], {"tensor": (t + k) % 8})

    def probabilities():
        total = lgs[0:4, :]
        for k in range(1, 8):
            cp.got(("lg", k))
            total = total + lgr[k][0:4, :]
        l0 = jnp.zeros((1, 128), F32)
        l1 = jnp.zeros((1, 128), F32)
        for j in range(4):
            l0 = l0 + jnp.where(e0 == j, total[j : j + 1, :], 0.0)
            l1 = l1 + jnp.where(e1 == j, total[j : j + 1, :], 0.0)
        p0 = jax.nn.sigmoid(l0 - l1)
        p1 = jax.nn.sigmoid(l1 - l0)
        picks.extend((p0, p1))
        low0 = p0.astype(BF16).astype(F32)
        low1 = p1.astype(BF16).astype(F32)
        col = jnp.sum(table0 * low0 + table1 * low1, axis=1, keepdims=True)
        pcol[0:CAP, :] = col
        prs[...] = jnp.broadcast_to(to_row(col), (8, 128))
        for k in (1, 7):
            cp.add(("pr", k), prs, prr.at[place(-k)], {"dp": (z + k) % 8})

    def far(d):
        for k in sorted({d, 8 - d}):
            cp.add(("ix", k), ix.at[0], ix.at[place(-k)], {"dp": (z + k) % 8})
            cp.add(("pr", k), prs, prr.at[place(-k)], {"dp": (z + k) % 8})

    def pass_on(d, half):
        for which in "tg":
            cp.got(("r", d, half, which))
        if d < 3 or half == 0:
            ring(d, half)
        for which in "tg":
            cp.got(("l", d, half, which))
        if d < 3 or half == 1:
            ring_back(d, half)

    def rows_in(k):
        u0, n = CHUNKS[k]
        return u0 * HALF, n * HALF

    def units_in(k):
        u0, n = CHUNKS[k]
        return UNITS[u0 : u0 + n]

    def halves(k):
        r0, r = rows_in(k)
        h = r // 2
        return slice(r0, r0 + h), slice(r0 + h, r0 + r), pl.ds(r0, h), pl.ds(r0 + h, h)

    blocks_seen, halves_seen = set(), set()

    ready = []

    def forward(k, j):
        r0, r = rows_in(k)
        if not ready:
            for w in wcopies:
                w.wait()
            ready.append(1)
        for o, half in units_in(k):
            if j == 2 and o == 4:
                for which in "tg":
                    cp.got(("rl"[half], 4, half, which))
        a = tk[r0 : r0 + r, :]
        b = gr[r0 : r0 + r, :]
        q = turn[j]
        cols = pl.ds(pl.multiple_of(q * 256, 256), 256)
        for m, v in enumerate((
            dot_nn(a, gw[:, cols]), dot_nn(a, uw[:, cols]), dot_nt(b, dw[cols, :]),
        )):
            v = v.astype(BF16)
            part[0, q, r0 : r0 + r, m * 128 : m * 128 + 128] = v[:, 0:128]
            part[1, q, r0 : r0 + r, m * 128 : m * 128 + 128] = v[:, 128:256]

    def to_sibling(k, j):
        r0, r = rows_in(k)
        rows = pl.ds(r0, r)
        q = turn[j]
        cp.add(("d", k, j), part.at[1 - c, q, rows, :], dbuf.at[q, rows, :], {"tensor": t_sib})

    def fold(target, rows, extra=None):
        v = part[c, target, rows, :].astype(F32) + dbuf[target, rows, :].astype(F32)
        if extra is not None:
            v = v + extra[rows, :].astype(F32)
        part[c, target, rows, :] = v.astype(BF16)

    def reduce_1(k, j):
        sa, sb, da, db = halves(k)
        cp.got(("d", k, j))
        if j == 2:
            fold(across, sa)
            cp.add(("fa", k), part.at[c, across, da, :], fa.at[da, :], {"tensor": t_right})
            fold(across, sb)
            cp.add(("fb", k), part.at[c, across, db, :], fb.at[db, :], {"tensor": t_left})
        if j == 1:
            fold(right, sb)
            cp.add(("rlb", k), part.at[c, right, db, :], rl.at[db, :], {"tensor": t_right})
        if j == 3:
            fold(left, sa)
            cp.add(("rra", k), part.at[c, left, da, :], rr.at[da, :], {"tensor": t_left})

    def reduce_2(k, side):
        sa, sb, da, db = halves(k)
        if side == 0:
            cp.got(("fa", k))
            fold(right, sa, fa)
            cp.add(("rla", k), part.at[c, right, da, :], rl.at[da, :], {"tensor": t_right})
        else:
            cp.got(("fb", k))
            fold(left, sb, fb)
            cp.add(("rrb", k), part.at[c, left, db, :], rr.at[db, :], {"tensor": t_left})

    def tcols(q):
        return pl.ds(pl.multiple_of(q * 128, 128), 128)

    def h_copy(name, rows, q, device):
        ref = hh.at[:, rows, tcols(q)]
        cp.add(name, ref, ref, {"tensor": device})

    def activate(k):
        sa, sb, da, db = halves(k)
        for o, half in units_in(k):
            if o != 0 and o not in blocks_seen:
                blocks_seen.add(o)
                cp.got(("pr", (-o) % 8))
                col = to_col(prr[POS[o]][0:1, :])
                for i in range(2):
                    pcol[ROW[o, i] : ROW[o, i] + HALF, :] = col[i * HALF : (i + 1) * HALF, :]
        cp.got(("d", k, 0))
        sums = []
        for s, names in ((sb, ("rlb", "rrb")), (sa, ("rla", "rra"))):
            for q in names:
                cp.got((q, k))
            v = part[c, x, s, :].astype(F32) + dbuf[x, s, :].astype(F32)
            v = v + rl[s, :].astype(F32) + rr[s, :].astype(F32)
            gate, up, ga = v[:, 0:128], v[:, 128:256], v[:, 256:384]
            g = jax.nn.sigmoid(gate)
            hid = (gate * g * up).astype(BF16)
            a = pcol[s, :] * ga
            hh[0, s, tcols(t)] = hid
            hh[1, s, tcols(t)] = (a * up * g * (1.0 + gate * (1.0 - g))).astype(BF16)
            hh[2, s, tcols(t)] = (a * gate * g).astype(BF16)
            sums.insert(0, jnp.sum(hid.astype(F32) * ga, axis=1, keepdims=True))
        h_copy(("ra", k), da, t, t_right)
        h_copy(("lb", k), db, t, t_left)
        h_copy(("rb", k), db, t, t_right)
        h_copy(("la", k), da, t, t_left)
        h_copy(("so", k), pl.ds(*rows_in(k)), t, t_sib)
        dcol[sa, :] = sums[0]
        dcol[sb, :] = sums[1]
        for o, half in units_in(k):
            halves_seen.add((o, half))
            if (o, 1 - half) in halves_seen:
                col = jnp.concatenate(
                    [dcol[ROW[o, i] : ROW[o, i] + HALF, :] for i in range(2)], axis=0)
                p = POS[o]
                dps[p] = jnp.broadcast_to(to_row(col), (8, 128))
                if o != 0:
                    cp.add(("dp", o), dps.at[p], dpr.at[place(-o)], {"dp": (z + o) % 8})
        r0, r = rows_in(k)
        s = slice(r0, r0 + r)
        sc[s, :] = (pcol[s, :] * gr[s, :].astype(F32)).astype(BF16)

    def spread(k, i):
        sa, sb, da, db = halves(k)
        full = pl.ds(*rows_in(k))
        if i == 0:
            cp.got(("ra", k))
            h_copy(("xa", k), da, t_left, t_right)
        if i == 1:
            cp.got(("lb", k))
            h_copy(("xb", k), db, t_right, t_left)
        if i == 2:
            cp.got(("rb", k))
            h_copy(("sl", k), full, t_left, t_sib)
        if i == 3:
            cp.got(("la", k))
            h_copy(("sr", k), full, t_right, t_sib)
        if i == 4:
            cp.got(("xa", k))
            cp.got(("xb", k))
            h_copy(("sx", k), full, across * 2 + c, t_sib)

    def tables(p):
        o = BLOCKS[p]
        if o != 0:
            cp.got(("ix", (-o) % 8))
        v = ix[p]
        both = table(v[0:1, :], v[2:3, :]) + table(v[1:2, :], v[3:4, :])
        selt[p] = both.T.astype(BF16)

    def chunks_in(m):
        k0, n = BACKS[m]
        return range(k0, k0 + n)

    def blocks_in(m):
        return [o for k in chunks_in(m) for o, half in units_in(k) if half == 0]

    def backward(m):
        for k in chunks_in(m):
            for q in ("so", "sl", "sr", "sx"):
                cp.got((q, k))
        r0 = rows_in(chunks_in(m)[0])[0]
        r = sum(rows_in(k)[1] for k in chunks_in(m))
        a = hh[1, r0 : r0 + r, :]
        b = hh[2, r0 : r0 + r, :]
        for i in range(3):
            cols = slice(i * 256, i * 256 + 256)
            dxs[r0 : r0 + r, cols] = (dot_nt(a, gw[cols, :]) + dot_nt(b, uw[cols, :])).astype(BF16)
        for i, o in enumerate(blocks_in(m)):
            v = jnp.concatenate([dxs[ROW[o, h] : ROW[o, h] + HALF, :] for h in range(2)], axis=0)
            yd[m][i] = dot_nn(selt[POS[o]], v).astype(BF16)

        def piece(q, low):
            return yd[m].at[:, pl.ds(pl.multiple_of(((y + q) % 4) * 32 + low, 16), 16), :]

        cp.add(("ya", m), piece(2, 0), ya[m], {"expert": (y + 1) % 4})
        cp.add(("yb", m), piece(2, 16), yb[m], {"expert": (y + 3) % 4})
        cp.add(("yr", m), piece(1, 16), yr[m].at[:, pl.ds(16, 16), :], {"expert": (y + 1) % 4})
        cp.add(("yl", m), piece(3, 0), yl[m].at[:, pl.ds(0, 16), :], {"expert": (y + 3) % 4})

    def relay(m):
        for name, q, low, buf, put in (("ya", 1, 0, ya, yr), ("yb", 3, 16, yb, yl)):
            cp.got((name, m))
            rows = pl.ds(pl.multiple_of(((y + q) % 4) * 32 + low, 16), 16)
            for i in range(len(blocks_in(m))):
                yd[m][i, rows, :] = (
                    yd[m][i, rows, :].astype(F32) + buf[m][i].astype(F32)).astype(BF16)
            cp.add((name, m, 2), yd[m].at[:, rows, :], put[m].at[:, pl.ds(low, 16), :],
                   {"expert": (y + q) % 4})

    def homeward(m):
        for name in (("yr", m), ("yl", m), ("ya", m, 2), ("yb", m, 2)):
            cp.got(name)
        rows = pl.ds(pl.multiple_of(y * 32, 32), 32)
        for i, o in enumerate(blocks_in(m)):
            v = yd[m][i, rows, :].astype(F32) + yr[m][i].astype(F32) + yl[m][i].astype(F32)
            if o == 0:
                own_q[...] = v
            else:
                yq[POS[o]] = v.astype(BF16)
                cp.add(("z", o), yq.at[POS[o]], zq.at[place(-o)], {"dp": (z + o) % 8})

    def router_1():
        total = dps[0][0:1, :]
        for p in range(8):
            if BLOCKS[p] != 0:
                o = BLOCKS[p]
                cp.got(("dp", -o if o != 4 else 4))
                total = total + dpr[p][0:1, :]
        col = to_col(total)
        pts[...] = rows8(jnp.sum(table0 * col, axis=0, keepdims=True),
                         jnp.sum(table1 * col, axis=0, keepdims=True))
        for k in range(1, 32):
            cp.add(("pt", k), pts, ptr.at[k],
                   {"expert": (y + k // 8) % 4, "tensor": (t + k) % 8})

    def router_3():
        total = pts[...]
        for k in range(1, 32):
            cp.got(("pt", k))
        for k in range(1, 32):
            total = total + ptr[k]
        d0, d1 = total[0:1, :], total[1:2, :]
        p0, p1 = picks
        mixed = p0 * d0 + p1 * d1
        w0 = p0 * (d0 - mixed)
        w1 = p1 * (d1 - mixed)
        grads = [jnp.where(e0 == j, w0, 0.0) + jnp.where(e1 == j, w1, 0.0) for j in range(4)]
        split = [parts3(v) for v in grads]
        row = lax.broadcasted_iota(jnp.int32, (16, 128), 0)
        lhs = jnp.zeros((16, 128), F32)
        for i in range(3):
            for j in range(4):
                lhs = jnp.where(row == i * 4 + j, split[j][i].astype(F32), lhs)
        v = dot_nn(lhs.astype(BF16), tok_in[...])
        rgs[...] = v[0:4, :] + v[4:8, :] + v[8:12, :]
        for k in range(1, 8):
            cp.add(("rg", k), rgs, rgr.at[k], {"dp": (z + k) % 8})
        i0 = lax.broadcasted_iota(jnp.int32, (128, 128), 0)
        i1 = lax.broadcasted_iota(jnp.int32, (128, 128), 1)
        eye_t = (i0 == i1).astype(F32)

        def col_t(row):
            return jnp.sum(eye_t * row, axis=1, keepdims=True)

        lane = lax.broadcasted_iota(jnp.int32, (128, 16), 1)
        of_expert = (lane % 4).astype(F32)
        v = (jnp.where(col_t(e0.astype(F32)) == of_expert, col_t(w0), 0.0)
             + jnp.where(col_t(e1.astype(F32)) == of_expert, col_t(w1), 0.0))
        hi, mid, low = (q.astype(F32) for q in parts3(v))
        lg3[...] = jnp.where(lane < 4, hi, jnp.where(lane < 8, mid, jnp.where(lane < 12, low, 0.0)))

    def router_5():
        total = rgs[...]
        for k in range(1, 8):
            cp.got(("rg", k))
            total = total + rgr[k]
        router_out[...] = total

    def finish():
        rows = pl.ds(pl.multiple_of(y * 32, 32), 32)
        total = own_q[...]
        total = total + dot_nn(lg3[rows, :].astype(BF16), jnp.concatenate([rwt[...]] * 4, axis=0))
        for p in range(8):
            o = BLOCKS[p]
            if o != 0:
                cp.got(("z", -o if o != 4 else 4))
                total = total + zq[p].astype(F32)
        tok_out[...] = total.astype(BF16)

    def weights(m, i):
        out, left_side, right_side = (
            (gg_o, tk, hh.at[1]), (ug_o, tk, hh.at[2]), (dg_o, hh.at[0], sc))[m]
        size = out.shape[0] // 3 if m < 2 else out.shape[0] // 4
        rows = slice(i * size, i * size + size)
        out[rows, :] = lax.dot_general(
            left_side[:, rows], right_side[...], (((0,), (0,)), ((), ())),
            preferred_element_type=F32).astype(BF16)

    run = {
        "open": open_up, "prob": probabilities, "far": far, "Z": pass_on, "F": forward, "D": to_sibling,
        "R1": reduce_1, "R2": reduce_2, "E": activate, "G": spread, "X": backward,
        "Y": homeward, "P1": router_1, "P3": router_3,
        "P5": router_5, "S": tables, "V": relay, "W": weights, "end": finish,
    }
    for step in STEPS:
        run[step[0]](*step[1:])
    cp.drain()


def put_out(*refs):
    sem = refs[10]
    copies = [pltpu.make_async_copy(refs[i], refs[5 + i], sem.at[i]) for i in range(5)]
    for q in copies:
        q.start()
    for q in copies:
        q.wait()


def shards(
    tokens, out_grad, router_weight, gate_weight, up_weight, down_weight, expert_index, slot_index
):
    vm = pl.BlockSpec(memory_space=pltpu.VMEM)
    hbm = pl.BlockSpec(memory_space=pltpu.HBM)
    V = pltpu.VMEM
    small = V((8, 128), F32)
    several = V((8, 8, 128), F32)
    out_shape = [
        jax.ShapeDtypeStruct((32, 768), BF16),
        jax.ShapeDtypeStruct((4, 768), F32),
        jax.ShapeDtypeStruct((768, 1024), BF16),
        jax.ShapeDtypeStruct((768, 1024), BF16),
        jax.ShapeDtypeStruct((1024, 768), BF16),
    ]
    results = pl.pallas_call(
        kernel,
        name="moe_backward",
        in_specs=[hbm] * 8,
        out_specs=[vm] * 5,
        out_shape=out_shape,
        scratch_shapes=[
            V((768, 768), BF16), V((768, 768), BF16), V((768, 768), BF16),
            V((768, 1024), BF16), V((768, 1024), BF16), V((1024, 768), BF16),
            V((2, 4, 768, 384), BF16), V((4, 768, 384), BF16),
            V((768, 384), BF16), V((768, 384), BF16), V((768, 384), BF16), V((768, 384), BF16),
            V((3, 768, 1024), BF16), V((768, 1), F32), V((768, 1), F32),
            small, several, small, several, several, several, V((8, 8, 128), jnp.int32),
            V((8, 128, CAP), BF16), V((768, 768), BF16), V((8, 32, 768), BF16),
            V((8, 32, 768), BF16), V((32, 768), F32),
            small, V((32, 8, 128), F32), V((4, 768), F32), V((8, 4, 768), F32), V((128, 16), F32),
            V((128, 768), BF16), V((128, 768), BF16), V((4, 768), BF16),
            V((2, 128), jnp.int32), V((2, 128), jnp.int32),
            pltpu.SemaphoreType.DMA((N_COPIES,)), pltpu.SemaphoreType.DMA((N_COPIES,)),
            pltpu.SemaphoreType.DMA((8,)),
            *(V((sum(GROUPS[k0 : k0 + n]) // 2, rows, 768), BF16)
              for rows in (128, 16, 16, 32, 32) for k0, n in BACKS),
        ],
        compiler_params=pltpu.CompilerParams(
            collective_id=0, has_side_effects=True, vmem_limit_bytes=40 * 1024 * 1024
        ),
    )(
        *(pltpu.with_memory_space_constraint(v, pltpu.HBM) for v in (
            tokens, out_grad, router_weight.T, expert_index.T, slot_index.T,
            gate_weight[0], up_weight[0], down_weight[0],
        ))
    )
    tokens_grad, router_grad, gate_grad, up_grad, down_grad = pl.pallas_call(
        put_out,
        name="put_out",
        in_specs=[vm] * 5,
        out_specs=[hbm] * 5,
        out_shape=out_shape,
        scratch_shapes=[pltpu.SemaphoreType.DMA((5,))],
        compiler_params=pltpu.CompilerParams(vmem_limit_bytes=1024 * 1024),
    )(*results)
    return (tokens_grad, router_grad.T, gate_grad[None], up_grad[None], down_grad[None])


def solution(mesh):
    in_specs = (
        P("dp", "tensor"),
        P("dp", "tensor"),
        P("tensor", None),
        P("expert", "tensor", "dp"),
        P("expert", "tensor", "dp"),
        P("expert", "dp", "tensor"),
        P("dp", None),
        P("dp", None),
    )
    out_specs = (
        P(("dp", "expert"), "tensor"),
        P("tensor", None),
        P("expert", "tensor", "dp"),
        P("expert", "tensor", "dp"),
        P("expert", "dp", "tensor"),
    )
    return jax.shard_map(shards, mesh=mesh, in_specs=in_specs, out_specs=out_specs, check_vma=False)
```

```python
import jax
import jax.numpy as jnp
from jax import lax
from jax.experimental import pallas as pl
from jax.experimental.pallas import tpu as pltpu
from jax.sharding import PartitionSpec as P

CAP = 96
MESH = pl.DeviceIdType.MESH
F32 = jnp.float32
BF16 = jnp.bfloat16

UNITS = ((0, 0), (0, 1), (-1, 0), (1, 0), (-1, 1), (1, 1), (-2, 0), (2, 0), (-2, 1), (2, 1), (4, 0), (4, 1), (-3, 0), (-3, 1), (3, 0), (3, 1))
GROUPS = (2, 2, 2, 2, 2, 2, 2, 2)
BACK = (1, 2, 2, 1, 1, 1)
HALF = CAP // 2
BLOCKS = (0, -1, 1, -2, 2, -3, 3, 4)
POS = {o: i for i, o in enumerate(BLOCKS)}
ROW = {u: i * HALF for i, u in enumerate(UNITS)}


def near(offset):
    o = offset % 8
    return o if o <= 4 else o - 8


def place(offset):
    return POS[near(offset)]


def runs(sizes):
    ends = [sum(sizes[: i + 1]) for i in range(len(sizes))]
    return [(e - n, n) for e, n in zip(ends, sizes)]


CHUNKS = runs(GROUPS)
BACKS = runs(BACK)

STEPS = (
    ("open",), ("F", 0, 2), ("D", 0, 2), ("F", 0, 1), ("D", 0, 1), ("F", 0, 3), ("D", 0, 3),
    ("F", 0, 0), ("D", 0, 0), ("S", 0), ("R1", 0, 2), ("R1", 0, 1), ("R1", 0, 3), ("R2", 0, 0),
    ("R2", 0, 1), ("Z", 1, 0), ("prob",), ("far", 2), ("F", 1, 2), ("D", 1, 2), ("F", 1, 1),
    ("D", 1, 1), ("F", 1, 3), ("D", 1, 3), ("F", 1, 0), ("D", 1, 0), ("R1", 1, 2), ("R1", 1, 1),
    ("E", 0), ("R1", 1, 3), ("Z", 1, 1), ("F", 2, 2), ("D", 2, 2), ("F", 2, 1), ("D", 2, 1),
    ("F", 2, 3), ("D", 2, 3), ("F", 2, 0), ("D", 2, 0), ("S", 1), ("S", 2), ("R1", 2, 2),
    ("R2", 1, 0), ("R2", 1, 1), ("R1", 2, 1), ("R1", 2, 3), ("G", 0, 1), ("Z", 2, 0), ("far", 3),
    ("F", 3, 2), ("D", 3, 2), ("G", 0, 0), ("G", 0, 3), ("F", 3, 1), ("D", 3, 1), ("F", 3, 3),
    ("D", 3, 3), ("G", 0, 2), ("F", 3, 0), ("D", 3, 0), ("R1", 3, 2), ("R2", 2, 0), ("R2", 2, 1),
    ("R1", 3, 1), ("E", 1), ("Z", 2, 1), ("R1", 3, 3), ("F", 4, 2), ("D", 4, 2), ("F", 4, 1),
    ("D", 4, 1), ("F", 4, 3), ("D", 4, 3), ("G", 0, 4), ("F", 4, 0), ("D", 4, 0), ("S", 3),
    ("S", 4), ("R1", 4, 2), ("R2", 3, 0), ("R2", 3, 1), ("R1", 4, 1), ("R1", 4, 3), ("E", 2),
    ("Z", 3, 0), ("far", 4), ("G", 1, 1), ("X", 0), ("G", 1, 0), ("G", 1, 3), ("G", 1, 2),
    ("R2", 4, 0), ("R2", 4, 1), ("Z", 3, 1), ("E", 3), ("G", 2, 0), ("G", 2, 1), ("V", 0),
    ("G", 2, 2), ("G", 2, 3), ("G", 1, 4), ("E", 4), ("G", 3, 0), ("G", 3, 1), ("F", 5, 2),
    ("D", 5, 2), ("Y", 0), ("G", 3, 2), ("G", 3, 3), ("F", 5, 1), ("D", 5, 1), ("F", 5, 3),
    ("D", 5, 3), ("G", 2, 4), ("F", 5, 0), ("D", 5, 0), ("R1", 5, 2), ("F", 6, 2), ("D", 6, 2),
    ("F", 6, 1), ("D", 6, 1), ("G", 4, 0), ("G", 4, 1), ("F", 6, 3), ("D", 6, 3), ("R1", 5, 1),
    ("F", 6, 0), ("D", 6, 0), ("G", 4, 2), ("G", 4, 3), ("R1", 5, 3), ("F", 7, 2), ("D", 7, 2),
    ("G", 3, 4), ("R1", 6, 2), ("R1", 6, 1), ("R2", 5, 0), ("R2", 5, 1), ("R1", 6, 3), ("X", 1),
    ("G", 4, 4), ("R1", 7, 2), ("F", 7, 1), ("D", 7, 1), ("F", 7, 3), ("D", 7, 3), ("R2", 6, 0),
    ("R2", 6, 1), ("F", 7, 0), ("D", 7, 0), ("S", 5), ("R1", 7, 1), ("R1", 7, 3), ("E", 5),
    ("R2", 7, 0), ("R2", 7, 1), ("X", 2), ("E", 6), ("V", 1), ("S", 6), ("S", 7), ("G", 5, 0),
    ("G", 5, 1), ("G", 5, 2), ("G", 5, 3), ("E", 7), ("G", 6, 0), ("G", 6, 1), ("V", 2),
    ("G", 6, 2), ("G", 6, 3), ("G", 5, 4), ("Y", 1), ("G", 7, 0), ("G", 7, 1), ("X", 3),
    ("G", 7, 2), ("G", 6, 4), ("G", 7, 3), ("Y", 2), ("P1",), ("G", 7, 4), ("X", 4), ("V", 3),
    ("X", 5), ("W", 0, 0), ("P3",), ("W", 0, 1), ("V", 4), ("W", 0, 2), ("W", 1, 0), ("Y", 3),
    ("W", 1, 1), ("V", 5), ("W", 1, 2), ("W", 2, 0), ("W", 2, 1), ("Y", 4), ("W", 2, 2),
    ("W", 2, 3), ("Y", 5), ("P5",), ("end",),
)


def dot_nt(a, b):
    return lax.dot_general(a, b, (((1,), (1,)), ((), ())), preferred_element_type=F32)


def dot_nn(a, b):
    return lax.dot_general(a, b, (((1,), (0,)), ((), ())), preferred_element_type=F32)


class Copies:
    def __init__(self, send, recv):
        self.send, self.recv, self.at, self.made, self.sent = send, recv, {}, {}, []

    def describe(self, key, src, dst, device, slot):
        i = self.at.setdefault(key, len(self.at))
        return pltpu.make_async_remote_copy(
            src_ref=src,
            dst_ref=dst,
            send_sem=self.send.at[slot],
            recv_sem=self.recv.at[i],
            device_id=device,
            device_id_type=MESH,
        )

    def add(self, name, src, dst, device, group=None):
        slot = len(self.sent) % N_SEND
        if len(self.sent) >= N_SEND:
            self.sent[-N_SEND].wait_send()
        c = self.describe(group or name, src, dst, device, slot)
        self.sent.append(c)
        self.made[name] = c
        c.start()

    def got(self, name):
        self.made[name].wait_recv()

    def got_all(self, group, ref, device):
        self.describe(group, ref, ref, device, 0).wait_recv()

    def drain(self):
        for c in self.sent[-N_SEND:]:
            c.wait_send()


N_SEND = 32
N_RECV = 155


def kernel(
    tok_h, og_h, rwt_h, ex_h, sl_h, gw_h, uw_h, dw_h,
    tok_out, router_out, gg_o, ug_o, dg_o,
    tk, gr, sc, gw, uw, dw, part, dbuf, fa, fb, rl, rr, hh, pcol, dcol,
    lgs, lgr, prs, prr, dps, dpr, ix, selt, dxs, yq, zq, own_q,
    pts, ptr, rgs, rgr, lg3,
    tok_in, og_in, rwt, ex, sl, send_sem, recv_sem, wsem, *sums,
):
    yd, ya, yb, yr, yl = (sums[i * len(BACKS) : (i + 1) * len(BACKS)] for i in range(5))
    z = lax.axis_index("dp")
    y = lax.axis_index("expert")
    t = lax.axis_index("tensor")
    x = t // 2
    c = t % 2
    right, left, across = (x + 1) % 4, (x + 3) % 4, (x + 2) % 4
    turn = (x, right, across, left)
    t_right, t_left, t_sib = right * 2 + c, left * 2 + c, x * 2 + (1 - c)

    loads = [
        pltpu.make_async_copy(a, b, wsem.at[i])
        for i, (a, b) in enumerate((
            (ex_h, ex), (sl_h, sl), (tok_h, tok_in), (og_h, og_in), (rwt_h, rwt),
            (gw_h, gw), (uw_h, uw), (dw_h, dw),
        ))
    ]
    for w in loads:
        w.start()
    wcopies = loads[5:]

    barrier = pltpu.get_barrier_semaphore()
    for k in (1, 7):
        pl.semaphore_signal(barrier, inc=1, device_id={"dp": (z + k) % 8}, device_id_type=MESH)
    for k in range(1, 32):
        pl.semaphore_signal(
            barrier, inc=1, device_id={"expert": (y + k // 8) % 4, "tensor": (t + k) % 8},
            device_id_type=MESH)

    cp = Copies(send_sem, recv_sem)

    for w in loads[:5]:
        w.wait()

    slot_at = lax.broadcasted_iota(jnp.int32, (CAP, 128), 0)
    lane_at = lax.broadcasted_iota(jnp.int32, (CAP, 128), 1)
    eye = (slot_at == lane_at).astype(F32)
    e0, e1, s0, s1 = ex[0:1, :], ex[1:2, :], sl[0:1, :], sl[1:2, :]

    def table(e, s):
        return jnp.where((e == y) & (s == slot_at), 1.0, 0.0).astype(F32)

    table0, table1 = table(e0, s0), table(e1, s1)
    select = (table0 + table1).astype(BF16)
    tk[0:CAP, :] = dot_nn(select, tok_in[...]).astype(BF16)
    gr[0:CAP, :] = dot_nn(select, og_in[...]).astype(BF16)
    lgs[4:8, :] = jnp.zeros((4, 128), F32)
    lgs[0:4, :] = dot_nt(rwt[...], tok_in[...])
    ix[0] = jnp.zeros((8, 128), jnp.int32)
    ix[0, 0:2, :] = ex[...]
    ix[0, 2:4, :] = sl[...]

    def ring(step, half):
        for which, buf in (("t", tk), ("g", gr)):
            cp.add(("r", step + 1, half, which), buf.at[pl.ds(ROW[near(-step), half], HALF)],
                   buf.at[pl.ds(ROW[near(-step - 1), half], HALF)], {"dp": (z + 1) % 8},
                   ("r", step + 1, half))

    def ring_back(step, half):
        for which, buf in (("t", tk), ("g", gr)):
            cp.add(("l", step + 1, half, which), buf.at[pl.ds(ROW[near(step), half], HALF)],
                   buf.at[pl.ds(ROW[near(step + 1), half], HALF)], {"dp": (z + 7) % 8},
                   ("l", step + 1, half))

    def piece_in(way, step, half):
        cp.got_all((way, step, half), tk.at[pl.ds(0, CAP)], {"dp": (z + 1) % 8})

    def to_col(row):
        return jnp.sum(eye * row, axis=1, keepdims=True)

    def to_row(col):
        return jnp.sum(eye * col, axis=0, keepdims=True)

    def parts3(v):
        hi = v.astype(BF16)
        rest = v - hi.astype(F32)
        mid = rest.astype(BF16)
        low = (rest - mid.astype(F32)).astype(BF16)
        return hi, mid, low

    def rows8(*given):
        row = lax.broadcasted_iota(jnp.int32, (8, 128), 0)
        v = jnp.zeros((8, 128), F32)
        for i, r in enumerate(given):
            v = jnp.where(row == i, r, v)
        return v

    picks = []

    def open_up():
        pl.semaphore_wait(barrier, 33)
        for k in (1, 7):
            cp.add(("ix", k), ix.at[0], ix.at[place(-k)], {"dp": (z + k) % 8})
        for half in range(2):
            ring(0, half)
            ring_back(0, half)
        for k in range(1, 8):
            cp.add(("lg", k), lgs, lgr.at[k], {"tensor": (t + k) % 8}, "lg")

    def probabilities():
        total = lgs[0:4, :]
        cp.got_all("lg", lgr.at[pl.ds(1, 7)], {"tensor": t_sib})
        for k in range(1, 8):
            total = total + lgr[k][0:4, :]
        l0 = jnp.zeros((1, 128), F32)
        l1 = jnp.zeros((1, 128), F32)
        for j in range(4):
            l0 = l0 + jnp.where(e0 == j, total[j : j + 1, :], 0.0)
            l1 = l1 + jnp.where(e1 == j, total[j : j + 1, :], 0.0)
        p0 = jax.nn.sigmoid(l0 - l1)
        p1 = jax.nn.sigmoid(l1 - l0)
        picks.extend((p0, p1))
        low0 = p0.astype(BF16).astype(F32)
        low1 = p1.astype(BF16).astype(F32)
        col = jnp.sum(table0 * low0 + table1 * low1, axis=1, keepdims=True)
        pcol[0:CAP, :] = col
        prs[...] = jnp.broadcast_to(to_row(col), (8, 128))
        for k in (1, 7):
            cp.add(("pr", k), prs, prr.at[place(-k)], {"dp": (z + k) % 8})

    def far(d):
        for k in sorted({d, 8 - d}):
            cp.add(("ix", k), ix.at[0], ix.at[place(-k)], {"dp": (z + k) % 8})
            cp.add(("pr", k), prs, prr.at[place(-k)], {"dp": (z + k) % 8})

    def pass_on(d, half):
        piece_in("r", d, half)
        if d < 3 or half == 0:
            ring(d, half)
        piece_in("l", d, half)
        if d < 3 or half == 1:
            ring_back(d, half)

    def rows_in(k):
        u0, n = CHUNKS[k]
        return u0 * HALF, n * HALF

    def units_in(k):
        u0, n = CHUNKS[k]
        return UNITS[u0 : u0 + n]

    def halves(k):
        r0, r = rows_in(k)
        h = r // 2
        return slice(r0, r0 + h), slice(r0 + h, r0 + r), pl.ds(r0, h), pl.ds(r0 + h, h)

    blocks_seen, halves_seen = set(), set()

    ready = []

    def forward(k, j):
        r0, r = rows_in(k)
        if not ready:
            for w in wcopies:
                w.wait()
            ready.append(1)
        for o, half in units_in(k):
            if j == 2 and o == 4:
                piece_in("rl"[half], 4, half)
        a = tk[r0 : r0 + r, :]
        b = gr[r0 : r0 + r, :]
        q = turn[j]
        cols = pl.ds(pl.multiple_of(q * 256, 256), 256)
        for m, v in enumerate((
            dot_nn(a, gw[:, cols]), dot_nn(a, uw[:, cols]), dot_nt(b, dw[cols, :]),
        )):
            v = v.astype(BF16)
            part[0, q, r0 : r0 + r, m * 128 : m * 128 + 128] = v[:, 0:128]
            part[1, q, r0 : r0 + r, m * 128 : m * 128 + 128] = v[:, 128:256]

    def to_sibling(k, j):
        r0, r = rows_in(k)
        rows = pl.ds(r0, r)
        q = turn[j]
        cp.add(("d", k, j), part.at[1 - c, q, rows, :], dbuf.at[q, rows, :], {"tensor": t_sib})

    def fold(target, rows, extra=None):
        v = part[c, target, rows, :].astype(F32) + dbuf[target, rows, :].astype(F32)
        if extra is not None:
            v = v + extra[rows, :].astype(F32)
        part[c, target, rows, :] = v.astype(BF16)

    def reduce_1(k, j):
        sa, sb, da, db = halves(k)
        cp.got(("d", k, j))
        if j == 2:
            fold(across, sa)
            cp.add(("fa", k), part.at[c, across, da, :], fa.at[da, :], {"tensor": t_right})
            fold(across, sb)
            cp.add(("fb", k), part.at[c, across, db, :], fb.at[db, :], {"tensor": t_left})
        if j == 1:
            fold(right, sb)
            cp.add(("rlb", k), part.at[c, right, db, :], rl.at[db, :], {"tensor": t_right}, ("rs", k))
        if j == 3:
            fold(left, sa)
            cp.add(("rra", k), part.at[c, left, da, :], rr.at[da, :], {"tensor": t_left}, ("rs", k))

    def reduce_2(k, side):
        sa, sb, da, db = halves(k)
        if side == 0:
            cp.got(("fa", k))
            fold(right, sa, fa)
            cp.add(("rla", k), part.at[c, right, da, :], rl.at[da, :], {"tensor": t_right}, ("rs", k))
        else:
            cp.got(("fb", k))
            fold(left, sb, fb)
            cp.add(("rrb", k), part.at[c, left, db, :], rr.at[db, :], {"tensor": t_left}, ("rs", k))

    def tcols(q):
        return pl.ds(pl.multiple_of(q * 128, 128), 128)

    def h_copy(name, rows, q, device, group=None):
        ref = hh.at[:, rows, tcols(q)]
        cp.add(name, ref, ref, {"tensor": device}, group)

    def activate(k):
        sa, sb, da, db = halves(k)
        for o, half in units_in(k):
            if o != 0 and o not in blocks_seen:
                blocks_seen.add(o)
                cp.got(("pr", (-o) % 8))
                col = to_col(prr[POS[o]][0:1, :])
                for i in range(2):
                    pcol[ROW[o, i] : ROW[o, i] + HALF, :] = col[i * HALF : (i + 1) * HALF, :]
        cp.got(("d", k, 0))
        sums = []
        cp.got_all(("rs", k), dbuf.at[pl.ds(0, 2), pl.ds(*rows_in(k)), :], {"tensor": t_sib})
        for s in (sb, sa):
            v = part[c, x, s, :].astype(F32) + dbuf[x, s, :].astype(F32)
            v = v + rl[s, :].astype(F32) + rr[s, :].astype(F32)
            gate, up, ga = v[:, 0:128], v[:, 128:256], v[:, 256:384]
            g = jax.nn.sigmoid(gate)
            hid = (gate * g * up).astype(BF16)
            a = pcol[s, :] * ga
            hh[0, s, tcols(t)] = hid
            hh[1, s, tcols(t)] = (a * up * g * (1.0 + gate * (1.0 - g))).astype(BF16)
            hh[2, s, tcols(t)] = (a * gate * g).astype(BF16)
            sums.insert(0, jnp.sum(hid.astype(F32) * ga, axis=1, keepdims=True))
        h_copy(("ra", k), da, t, t_right)
        h_copy(("lb", k), db, t, t_left)
        h_copy(("rb", k), db, t, t_right)
        h_copy(("la", k), da, t, t_left)
        h_copy(("so", k), pl.ds(*rows_in(k)), t, t_sib, ("s", k))
        dcol[sa, :] = sums[0]
        dcol[sb, :] = sums[1]
        for o, half in units_in(k):
            halves_seen.add((o, half))
            if (o, 1 - half) in halves_seen:
                col = jnp.concatenate(
                    [dcol[ROW[o, i] : ROW[o, i] + HALF, :] for i in range(2)], axis=0)
                p = POS[o]
                dps[p] = jnp.broadcast_to(to_row(col), (8, 128))
                if o != 0:
                    cp.add(("dp", o), dps.at[p], dpr.at[place(-o)], {"dp": (z + o) % 8}, "dp")
        r0, r = rows_in(k)
        s = slice(r0, r0 + r)
        sc[s, :] = (pcol[s, :] * gr[s, :].astype(F32)).astype(BF16)

    def spread(k, i):
        sa, sb, da, db = halves(k)
        full = pl.ds(*rows_in(k))
        if i == 0:
            cp.got(("ra", k))
            h_copy(("xa", k), da, t_left, t_right, ("x", k))
        if i == 1:
            cp.got(("lb", k))
            h_copy(("xb", k), db, t_right, t_left, ("x", k))
        if i == 2:
            cp.got(("rb", k))
            h_copy(("sl", k), full, t_left, t_sib, ("s", k))
        if i == 3:
            cp.got(("la", k))
            h_copy(("sr", k), full, t_right, t_sib, ("s", k))
        if i == 4:
            cp.got_all(("x", k), hh.at[:, full, pl.ds(0, 128)], {"tensor": t_sib})
            h_copy(("sx", k), full, across * 2 + c, t_sib, ("s", k))

    def tables(p):
        o = BLOCKS[p]
        if o != 0:
            cp.got(("ix", (-o) % 8))
        v = ix[p]
        both = table(v[0:1, :], v[2:3, :]) + table(v[1:2, :], v[3:4, :])
        selt[p] = both.T.astype(BF16)

    def chunks_in(m):
        k0, n = BACKS[m]
        return range(k0, k0 + n)

    def blocks_in(m):
        return [o for k in chunks_in(m) for o, half in units_in(k) if half == 0]

    def backward(m):
        for k in chunks_in(m):
            cp.got_all(("s", k), hh.at[:, pl.ds(*rows_in(k)), pl.ds(0, 512)], {"tensor": t_sib})
        r0 = rows_in(chunks_in(m)[0])[0]
        r = sum(rows_in(k)[1] for k in chunks_in(m))
        a = hh[1, r0 : r0 + r, :]
        b = hh[2, r0 : r0 + r, :]
        for i in range(3):
            cols = slice(i * 256, i * 256 + 256)
            dxs[r0 : r0 + r, cols] = (dot_nt(a, gw[cols, :]) + dot_nt(b, uw[cols, :])).astype(BF16)
        for i, o in enumerate(blocks_in(m)):
            v = jnp.concatenate([dxs[ROW[o, h] : ROW[o, h] + HALF, :] for h in range(2)], axis=0)
            yd[m][i] = dot_nn(selt[POS[o]], v).astype(BF16)

        def piece(q, low):
            return yd[m].at[:, pl.ds(pl.multiple_of(((y + q) % 4) * 32 + low, 16), 16), :]

        cp.add(("ya", m), piece(2, 0), ya[m], {"expert": (y + 1) % 4})
        cp.add(("yb", m), piece(2, 16), yb[m], {"expert": (y + 3) % 4})
        cp.add(("yr", m), piece(1, 16), yr[m].at[:, pl.ds(16, 16), :], {"expert": (y + 1) % 4},
               ("yy", m))
        cp.add(("yl", m), piece(3, 0), yl[m].at[:, pl.ds(0, 16), :], {"expert": (y + 3) % 4},
               ("yy", m))

    def relay(m):
        for name, q, low, buf, put in (("ya", 1, 0, ya, yr), ("yb", 3, 16, yb, yl)):
            cp.got((name, m))
            rows = pl.ds(pl.multiple_of(((y + q) % 4) * 32 + low, 16), 16)
            for i in range(len(blocks_in(m))):
                yd[m][i, rows, :] = (
                    yd[m][i, rows, :].astype(F32) + buf[m][i].astype(F32)).astype(BF16)
            cp.add((name, m, 2), yd[m].at[:, rows, :], put[m].at[:, pl.ds(low, 16), :],
                   {"expert": (y + q) % 4}, ("yy", m))

    def homeward(m):
        n = len(blocks_in(m))
        cp.got_all(("yy", m), yd[m].at[pl.ds(0, n), pl.ds(0, 64), :], {"expert": (y + 1) % 4})
        rows = pl.ds(pl.multiple_of(y * 32, 32), 32)
        for i, o in enumerate(blocks_in(m)):
            v = yd[m][i, rows, :].astype(F32) + yr[m][i].astype(F32) + yl[m][i].astype(F32)
            if o == 0:
                own_q[...] = v
            else:
                yq[POS[o]] = v.astype(BF16)
                cp.add(("z", o), yq.at[POS[o]], zq.at[place(-o)], {"dp": (z + o) % 8}, "z")

    def router_1():
        total = dps[0][0:1, :]
        cp.got_all("dp", dpr.at[pl.ds(1, 7)], {"dp": (z + 1) % 8})
        for p in range(1, 8):
            total = total + dpr[p][0:1, :]
        col = to_col(total)
        pts[...] = rows8(jnp.sum(table0 * col, axis=0, keepdims=True),
                         jnp.sum(table1 * col, axis=0, keepdims=True))
        for k in range(1, 32):
            cp.add(("pt", k), pts, ptr.at[k],
                   {"expert": (y + k // 8) % 4, "tensor": (t + k) % 8}, "pt")

    def router_3():
        total = pts[...]
        cp.got_all("pt", ptr.at[pl.ds(1, 31)], {"tensor": t_sib})
        for k in range(1, 32):
            total = total + ptr[k]
        d0, d1 = total[0:1, :], total[1:2, :]
        p0, p1 = picks
        mixed = p0 * d0 + p1 * d1
        w0 = p0 * (d0 - mixed)
        w1 = p1 * (d1 - mixed)
        grads = [jnp.where(e0 == j, w0, 0.0) + jnp.where(e1 == j, w1, 0.0) for j in range(4)]
        split = [parts3(v) for v in grads]
        row = lax.broadcasted_iota(jnp.int32, (16, 128), 0)
        lhs = jnp.zeros((16, 128), F32)
        for i in range(3):
            for j in range(4):
                lhs = jnp.where(row == i * 4 + j, split[j][i].astype(F32), lhs)
        v = dot_nn(lhs.astype(BF16), tok_in[...])
        rgs[...] = v[0:4, :] + v[4:8, :] + v[8:12, :]
        for k in range(1, 8):
            cp.add(("rg", k), rgs, rgr.at[k], {"dp": (z + k) % 8}, "rg")
        i0 = lax.broadcasted_iota(jnp.int32, (128, 128), 0)
        i1 = lax.broadcasted_iota(jnp.int32, (128, 128), 1)
        eye_t = (i0 == i1).astype(F32)

        def col_t(row):
            return jnp.sum(eye_t * row, axis=1, keepdims=True)

        lane = lax.broadcasted_iota(jnp.int32, (128, 16), 1)
        of_expert = (lane % 4).astype(F32)
        v = (jnp.where(col_t(e0.astype(F32)) == of_expert, col_t(w0), 0.0)
             + jnp.where(col_t(e1.astype(F32)) == of_expert, col_t(w1), 0.0))
        hi, mid, low = (q.astype(F32) for q in parts3(v))
        lg3[...] = jnp.where(lane < 4, hi, jnp.where(lane < 8, mid, jnp.where(lane < 12, low, 0.0)))

    def router_5():
        total = rgs[...]
        cp.got_all("rg", rgr.at[pl.ds(1, 7)], {"dp": (z + 1) % 8})
        for k in range(1, 8):
            total = total + rgr[k]
        router_out[...] = total

    def finish():
        cp.drain()
        rows = pl.ds(pl.multiple_of(y * 32, 32), 32)
        total = own_q[...]
        total = total + dot_nn(lg3[rows, :].astype(BF16), jnp.concatenate([rwt[...]] * 4, axis=0))
        cp.got_all("z", zq.at[pl.ds(1, 7)], {"dp": (z + 1) % 8})
        for p in range(1, 8):
            total = total + zq[p].astype(F32)
        tok_out[...] = total.astype(BF16)

    def weights(m, i):
        out, left_side, right_side = (
            (gg_o, tk, hh.at[1]), (ug_o, tk, hh.at[2]), (dg_o, hh.at[0], sc))[m]
        size = out.shape[0] // 3 if m < 2 else out.shape[0] // 4
        rows = slice(i * size, i * size + size)
        out[rows, :] = lax.dot_general(
            left_side[:, rows], right_side[...], (((0,), (0,)), ((), ())),
            preferred_element_type=F32).astype(BF16)

    run = {
        "open": open_up, "prob": probabilities, "far": far, "Z": pass_on, "F": forward, "D": to_sibling,
        "R1": reduce_1, "R2": reduce_2, "E": activate, "G": spread, "X": backward,
        "Y": homeward, "P1": router_1, "P3": router_3,
        "P5": router_5, "S": tables, "V": relay, "W": weights, "end": finish,
    }
    for step in STEPS:
        run[step[0]](*step[1:])


def put_out(*refs):
    sem = refs[10]
    copies = [pltpu.make_async_copy(refs[i], refs[5 + i], sem.at[i]) for i in range(5)]
    for q in copies:
        q.start()
    for q in copies:
        q.wait()


def shards(
    tokens, out_grad, router_weight, gate_weight, up_weight, down_weight, expert_index, slot_index
):
    vm = pl.BlockSpec(memory_space=pltpu.VMEM)
    hbm = pl.BlockSpec(memory_space=pltpu.HBM)
    V = pltpu.VMEM
    small = V((8, 128), F32)
    several = V((8, 8, 128), F32)
    out_shape = [
        jax.ShapeDtypeStruct((32, 768), BF16),
        jax.ShapeDtypeStruct((4, 768), F32),
        jax.ShapeDtypeStruct((768, 1024), BF16),
        jax.ShapeDtypeStruct((768, 1024), BF16),
        jax.ShapeDtypeStruct((1024, 768), BF16),
    ]
    results = pl.pallas_call(
        kernel,
        name="moe_backward",
        in_specs=[hbm] * 8,
        out_specs=[vm] * 5,
        out_shape=out_shape,
        scratch_shapes=[
            V((768, 768), BF16), V((768, 768), BF16), V((768, 768), BF16),
            V((768, 1024), BF16), V((768, 1024), BF16), V((1024, 768), BF16),
            V((2, 4, 768, 384), BF16), V((4, 768, 384), BF16),
            V((768, 384), BF16), V((768, 384), BF16), V((768, 384), BF16), V((768, 384), BF16),
            V((3, 768, 1024), BF16), V((768, 1), F32), V((768, 1), F32),
            small, several, small, several, several, several, V((8, 8, 128), jnp.int32),
            V((8, 128, CAP), BF16), V((768, 768), BF16), V((8, 32, 768), BF16),
            V((8, 32, 768), BF16), V((32, 768), F32),
            small, V((32, 8, 128), F32), V((4, 768), F32), V((8, 4, 768), F32), V((128, 16), F32),
            V((128, 768), BF16), V((128, 768), BF16), V((4, 768), BF16),
            V((2, 128), jnp.int32), V((2, 128), jnp.int32),
            pltpu.SemaphoreType.DMA((N_SEND,)), pltpu.SemaphoreType.DMA((N_RECV,)),
            pltpu.SemaphoreType.DMA((8,)),
            *(V((sum(GROUPS[k0 : k0 + n]) // 2, rows, 768), BF16)
              for rows in (128, 16, 16, 32, 32) for k0, n in BACKS),
        ],
        compiler_params=pltpu.CompilerParams(
            collective_id=0, has_side_effects=True, vmem_limit_bytes=40 * 1024 * 1024
        ),
    )(
        *(pltpu.with_memory_space_constraint(v, pltpu.HBM) for v in (
            tokens, out_grad, router_weight.T, expert_index.T, slot_index.T,
            gate_weight[0], up_weight[0], down_weight[0],
        ))
    )
    tokens_grad, router_grad, gate_grad, up_grad, down_grad = pl.pallas_call(
        put_out,
        name="put_out",
        in_specs=[vm] * 5,
        out_specs=[hbm] * 5,
        out_shape=out_shape,
        scratch_shapes=[pltpu.SemaphoreType.DMA((5,))],
        compiler_params=pltpu.CompilerParams(vmem_limit_bytes=1024 * 1024),
    )(*results)
    return (tokens_grad, router_grad.T, gate_grad[None], up_grad[None], down_grad[None])


def solution(mesh):
    in_specs = (
        P("dp", "tensor"),
        P("dp", "tensor"),
        P("tensor", None),
        P("expert", "tensor", "dp"),
        P("expert", "tensor", "dp"),
        P("expert", "dp", "tensor"),
        P("dp", None),
        P("dp", None),
    )
    out_specs = (
        P(("dp", "expert"), "tensor"),
        P("tensor", None),
        P("expert", "tensor", "dp"),
        P("expert", "tensor", "dp"),
        P("expert", "dp", "tensor"),
    )
    return jax.shard_map(shards, mesh=mesh, in_specs=in_specs, out_specs=out_specs, check_vma=False)
```

```python
import jax
import jax.numpy as jnp
from jax import lax
from jax.experimental import pallas as pl
from jax.experimental.pallas import tpu as pltpu
from jax.sharding import PartitionSpec as P

CAP = 96
MESH = pl.DeviceIdType.MESH
F32 = jnp.float32
BF16 = jnp.bfloat16

UNITS = ((0, 0), (0, 1), (-1, 0), (1, 0), (-1, 1), (1, 1), (-2, 0), (2, 0), (-2, 1), (2, 1), (4, 0), (4, 1), (-3, 0), (-3, 1), (3, 0), (3, 1))
GROUPS = (2, 2, 2, 2, 2, 2, 2, 2)
BACK = (1, 2, 2, 1, 1, 1)
HALF = CAP // 2
BLOCKS = (0, -1, 1, -2, 2, -3, 3, 4)
POS = {o: i for i, o in enumerate(BLOCKS)}
ROW = {u: i * HALF for i, u in enumerate(UNITS)}


def near(offset):
    o = offset % 8
    return o if o <= 4 else o - 8


def place(offset):
    return POS[near(offset)]


def runs(sizes):
    ends = [sum(sizes[: i + 1]) for i in range(len(sizes))]
    return [(e - n, n) for e, n in zip(ends, sizes)]


CHUNKS = runs(GROUPS)
BACKS = runs(BACK)

STEPS = (
    ("open",), ("F", 0, 2), ("D", 0, 2), ("F", 0, 1), ("D", 0, 1), ("F", 0, 3), ("D", 0, 3),
    ("F", 0, 0), ("D", 0, 0), ("S", 0), ("R1", 0, 2), ("R1", 0, 1), ("R1", 0, 3), ("R2", 0, 0),
    ("R2", 0, 1), ("Z", 1, 0), ("prob",), ("far", 2), ("F", 1, 2), ("D", 1, 2), ("F", 1, 1),
    ("D", 1, 1), ("F", 1, 3), ("D", 1, 3), ("F", 1, 0), ("D", 1, 0), ("R1", 1, 2), ("R1", 1, 1),
    ("E", 0), ("R1", 1, 3), ("Z", 1, 1), ("F", 2, 2), ("D", 2, 2), ("F", 2, 1), ("D", 2, 1),
    ("F", 2, 3), ("D", 2, 3), ("F", 2, 0), ("D", 2, 0), ("S", 1), ("S", 2), ("R1", 2, 2),
    ("R2", 1, 0), ("R2", 1, 1), ("R1", 2, 1), ("R1", 2, 3), ("G", 0, 1), ("Z", 2, 0), ("far", 3),
    ("F", 3, 2), ("D", 3, 2), ("G", 0, 0), ("G", 0, 3), ("F", 3, 1), ("D", 3, 1), ("F", 3, 3),
    ("D", 3, 3), ("G", 0, 2), ("F", 3, 0), ("D", 3, 0), ("R1", 3, 2), ("R2", 2, 0), ("R2", 2, 1),
    ("R1", 3, 1), ("E", 1), ("Z", 2, 1), ("R1", 3, 3), ("F", 4, 2), ("D", 4, 2), ("F", 4, 1),
    ("D", 4, 1), ("F", 4, 3), ("D", 4, 3), ("G", 0, 4), ("F", 4, 0), ("D", 4, 0), ("S", 3),
    ("S", 4), ("R1", 4, 2), ("R2", 3, 0), ("R2", 3, 1), ("R1", 4, 1), ("R1", 4, 3), ("E", 2),
    ("Z", 3, 0), ("far", 4), ("G", 1, 1), ("X", 0), ("G", 1, 0), ("G", 1, 3), ("G", 1, 2),
    ("R2", 4, 0), ("R2", 4, 1), ("Z", 3, 1), ("E", 3), ("G", 2, 0), ("G", 2, 1), ("V", 0),
    ("G", 2, 2), ("G", 2, 3), ("G", 1, 4), ("E", 4), ("G", 3, 0), ("G", 3, 1), ("F", 5, 2),
    ("D", 5, 2), ("Y", 0), ("G", 3, 2), ("G", 3, 3), ("F", 5, 1), ("D", 5, 1), ("F", 5, 3),
    ("D", 5, 3), ("G", 2, 4), ("F", 5, 0), ("D", 5, 0), ("R1", 5, 2), ("F", 6, 2), ("D", 6, 2),
    ("F", 6, 1), ("D", 6, 1), ("G", 4, 0), ("G", 4, 1), ("F", 6, 3), ("D", 6, 3), ("R1", 5, 1),
    ("F", 6, 0), ("D", 6, 0), ("G", 4, 2), ("G", 4, 3), ("R1", 5, 3), ("F", 7, 2), ("D", 7, 2),
    ("G", 3, 4), ("R1", 6, 2), ("R1", 6, 1), ("R2", 5, 0), ("R2", 5, 1), ("R1", 6, 3), ("X", 1),
    ("G", 4, 4), ("R1", 7, 2), ("F", 7, 1), ("D", 7, 1), ("F", 7, 3), ("D", 7, 3), ("R2", 6, 0),
    ("R2", 6, 1), ("F", 7, 0), ("D", 7, 0), ("S", 5), ("R1", 7, 1), ("R1", 7, 3), ("E", 5),
    ("R2", 7, 0), ("R2", 7, 1), ("X", 2), ("E", 6), ("V", 1), ("S", 6), ("S", 7), ("G", 5, 0),
    ("G", 5, 1), ("G", 5, 2), ("G", 5, 3), ("E", 7), ("G", 6, 0), ("G", 6, 1), ("V", 2),
    ("G", 6, 2), ("G", 6, 3), ("G", 5, 4), ("Y", 1), ("G", 7, 0), ("G", 7, 1), ("X", 3),
    ("G", 7, 2), ("G", 6, 4), ("G", 7, 3), ("Y", 2), ("G", 7, 4), ("P1",), ("X", 4), ("X", 5),
    ("W", 0, 0), ("Y", 3), ("W", 0, 1), ("W", 0, 2), ("V", 4), ("P3",), ("W", 1, 0), ("W", 1, 1),
    ("W", 1, 2), ("Y", 5), ("Y", 4), ("W", 2, 0), ("W", 2, 1), ("W", 2, 2), ("W", 2, 3), ("P5",),
    ("end",),
)


def dot_nt(a, b):
    return lax.dot_general(a, b, (((1,), (1,)), ((), ())), preferred_element_type=F32)


def dot_nn(a, b):
    return lax.dot_general(a, b, (((1,), (0,)), ((), ())), preferred_element_type=F32)


class Copies:
    def __init__(self, send, recv):
        self.send, self.recv, self.at, self.made, self.sent = send, recv, {}, {}, []

    def describe(self, key, src, dst, device, slot):
        i = self.at.setdefault(key, len(self.at))
        return pltpu.make_async_remote_copy(
            src_ref=src,
            dst_ref=dst,
            send_sem=self.send.at[slot],
            recv_sem=self.recv.at[i],
            device_id=device,
            device_id_type=MESH,
        )

    def add(self, name, src, dst, device, group=None):
        slot = len(self.sent) % N_SEND
        if group == "pt":
            slot = N_SEND
        elif len(self.sent) >= N_SEND:
            self.sent[-N_SEND].wait_send()
        c = self.describe(group or name, src, dst, device, slot)
        if slot < N_SEND:
            self.sent.append(c)
        self.made[name] = c
        c.start()

    def got(self, name):
        self.made[name].wait_recv()

    def got_all(self, group, ref, device):
        self.describe(group, ref, ref, device, 0).wait_recv()

    def drain(self):
        for c in self.sent[-N_SEND:]:
            c.wait_send()


DIRECT = (3, 5)
N_SEND = 40
N_RECV = 155


def kernel(
    tok_h, og_h, rwt_h, ex_h, sl_h, gw_h, uw_h, dw_h,
    tok_out, router_out, gg_o, ug_o, dg_o,
    tk, gr, sc, gw, uw, dw, part, dbuf, fa, fb, rl, rr, hh, pcol, dcol,
    lgs, lgr, prs, prr, dps, dpr, ix, selt, dxs, yq, zq, own_q,
    pts, ptr, rgs, rgr, lg3,
    tok_in, og_in, rwt, ex, sl, send_sem, recv_sem, wsem, *sums,
):
    yd, ya, yb, yr, yl, yx = (sums[i * len(BACKS) : (i + 1) * len(BACKS)] for i in range(6))
    z = lax.axis_index("dp")
    y = lax.axis_index("expert")
    t = lax.axis_index("tensor")
    x = t // 2
    c = t % 2
    right, left, across = (x + 1) % 4, (x + 3) % 4, (x + 2) % 4
    turn = (x, right, across, left)
    t_right, t_left, t_sib = right * 2 + c, left * 2 + c, x * 2 + (1 - c)

    loads = [
        pltpu.make_async_copy(a, b, wsem.at[i])
        for i, (a, b) in enumerate((
            (ex_h, ex), (sl_h, sl), (tok_h, tok_in), (og_h, og_in), (rwt_h, rwt),
            (gw_h, gw), (uw_h, uw), (dw_h, dw),
        ))
    ]
    for w in loads:
        w.start()
    wcopies = loads[5:]

    barrier = pltpu.get_barrier_semaphore()
    for k in (1, 7):
        pl.semaphore_signal(barrier, inc=1, device_id={"dp": (z + k) % 8}, device_id_type=MESH)
    for k in range(1, 32):
        pl.semaphore_signal(
            barrier, inc=1, device_id={"expert": (y + k // 8) % 4, "tensor": (t + k) % 8},
            device_id_type=MESH)

    cp = Copies(send_sem, recv_sem)

    for w in loads[:5]:
        w.wait()

    slot_at = lax.broadcasted_iota(jnp.int32, (CAP, 128), 0)
    lane_at = lax.broadcasted_iota(jnp.int32, (CAP, 128), 1)
    eye = (slot_at == lane_at).astype(F32)
    e0, e1, s0, s1 = ex[0:1, :], ex[1:2, :], sl[0:1, :], sl[1:2, :]

    def table(e, s):
        return jnp.where((e == y) & (s == slot_at), 1.0, 0.0).astype(F32)

    table0, table1 = table(e0, s0), table(e1, s1)
    select = (table0 + table1).astype(BF16)
    tk[0:CAP, :] = dot_nn(select, tok_in[...]).astype(BF16)
    gr[0:CAP, :] = dot_nn(select, og_in[...]).astype(BF16)
    lgs[4:8, :] = jnp.zeros((4, 128), F32)
    lgs[0:4, :] = dot_nt(rwt[...], tok_in[...])
    ix[0] = jnp.zeros((8, 128), jnp.int32)
    ix[0, 0:2, :] = ex[...]
    ix[0, 2:4, :] = sl[...]

    def ring(step, half):
        for which, buf in (("t", tk), ("g", gr)):
            cp.add(("r", step + 1, half, which), buf.at[pl.ds(ROW[near(-step), half], HALF)],
                   buf.at[pl.ds(ROW[near(-step - 1), half], HALF)], {"dp": (z + 1) % 8},
                   ("r", step + 1, half))

    def ring_back(step, half):
        for which, buf in (("t", tk), ("g", gr)):
            cp.add(("l", step + 1, half, which), buf.at[pl.ds(ROW[near(step), half], HALF)],
                   buf.at[pl.ds(ROW[near(step + 1), half], HALF)], {"dp": (z + 7) % 8},
                   ("l", step + 1, half))

    def piece_in(way, step, half):
        cp.got_all((way, step, half), tk.at[pl.ds(0, CAP)], {"dp": (z + 1) % 8})

    def to_col(row):
        return jnp.sum(eye * row, axis=1, keepdims=True)

    def to_row(col):
        return jnp.sum(eye * col, axis=0, keepdims=True)

    def parts3(v):
        hi = v.astype(BF16)
        rest = v - hi.astype(F32)
        mid = rest.astype(BF16)
        low = (rest - mid.astype(F32)).astype(BF16)
        return hi, mid, low

    def rows8(*given):
        row = lax.broadcasted_iota(jnp.int32, (8, 128), 0)
        v = jnp.zeros((8, 128), F32)
        for i, r in enumerate(given):
            v = jnp.where(row == i, r, v)
        return v

    picks = []

    def open_up():
        pl.semaphore_wait(barrier, 33)
        for k in (1, 7):
            cp.add(("ix", k), ix.at[0], ix.at[place(-k)], {"dp": (z + k) % 8})
        for half in range(2):
            ring(0, half)
            ring_back(0, half)
        for k in range(1, 8):
            cp.add(("lg", k), lgs, lgr.at[k], {"tensor": (t + k) % 8}, "lg")

    def probabilities():
        total = lgs[0:4, :]
        cp.got_all("lg", lgr.at[pl.ds(1, 7)], {"tensor": t_sib})
        for k in range(1, 8):
            total = total + lgr[k][0:4, :]
        l0 = jnp.zeros((1, 128), F32)
        l1 = jnp.zeros((1, 128), F32)
        for j in range(4):
            l0 = l0 + jnp.where(e0 == j, total[j : j + 1, :], 0.0)
            l1 = l1 + jnp.where(e1 == j, total[j : j + 1, :], 0.0)
        p0 = jax.nn.sigmoid(l0 - l1)
        p1 = jax.nn.sigmoid(l1 - l0)
        picks.extend((p0, p1))
        low0 = p0.astype(BF16).astype(F32)
        low1 = p1.astype(BF16).astype(F32)
        col = jnp.sum(table0 * low0 + table1 * low1, axis=1, keepdims=True)
        pcol[0:CAP, :] = col
        prs[...] = jnp.broadcast_to(to_row(col), (8, 128))
        for k in (1, 7):
            cp.add(("pr", k), prs, prr.at[place(-k)], {"dp": (z + k) % 8})

    def far(d):
        for k in sorted({d, 8 - d}):
            cp.add(("ix", k), ix.at[0], ix.at[place(-k)], {"dp": (z + k) % 8})
            cp.add(("pr", k), prs, prr.at[place(-k)], {"dp": (z + k) % 8})

    def pass_on(d, half):
        piece_in("r", d, half)
        if d < 3 or half == 0:
            ring(d, half)
        piece_in("l", d, half)
        if d < 3 or half == 1:
            ring_back(d, half)

    def rows_in(k):
        u0, n = CHUNKS[k]
        return u0 * HALF, n * HALF

    def units_in(k):
        u0, n = CHUNKS[k]
        return UNITS[u0 : u0 + n]

    def halves(k):
        r0, r = rows_in(k)
        h = r // 2
        return slice(r0, r0 + h), slice(r0 + h, r0 + r), pl.ds(r0, h), pl.ds(r0 + h, h)

    blocks_seen, halves_seen = set(), set()

    ready = []

    def forward(k, j):
        r0, r = rows_in(k)
        if not ready:
            for w in wcopies:
                w.wait()
            ready.append(1)
        for o, half in units_in(k):
            if j == 2 and o == 4:
                piece_in("rl"[half], 4, half)
        a = tk[r0 : r0 + r, :]
        b = gr[r0 : r0 + r, :]
        q = turn[j]
        cols = pl.ds(pl.multiple_of(q * 256, 256), 256)
        for m, v in enumerate((
            dot_nn(a, gw[:, cols]), dot_nn(a, uw[:, cols]), dot_nt(b, dw[cols, :]),
        )):
            v = v.astype(BF16)
            part[0, q, r0 : r0 + r, m * 128 : m * 128 + 128] = v[:, 0:128]
            part[1, q, r0 : r0 + r, m * 128 : m * 128 + 128] = v[:, 128:256]

    def to_sibling(k, j):
        r0, r = rows_in(k)
        rows = pl.ds(r0, r)
        q = turn[j]
        cp.add(("d", k, j), part.at[1 - c, q, rows, :], dbuf.at[q, rows, :], {"tensor": t_sib})

    def fold(target, rows, extra=None):
        v = part[c, target, rows, :].astype(F32) + dbuf[target, rows, :].astype(F32)
        if extra is not None:
            v = v + extra[rows, :].astype(F32)
        part[c, target, rows, :] = v.astype(BF16)

    def reduce_1(k, j):
        sa, sb, da, db = halves(k)
        cp.got(("d", k, j))
        if j == 2:
            fold(across, sa)
            cp.add(("fa", k), part.at[c, across, da, :], fa.at[da, :], {"tensor": t_right})
            fold(across, sb)
            cp.add(("fb", k), part.at[c, across, db, :], fb.at[db, :], {"tensor": t_left})
        if j == 1:
            fold(right, sb)
            cp.add(("rlb", k), part.at[c, right, db, :], rl.at[db, :], {"tensor": t_right}, ("rs", k))
        if j == 3:
            fold(left, sa)
            cp.add(("rra", k), part.at[c, left, da, :], rr.at[da, :], {"tensor": t_left}, ("rs", k))

    def reduce_2(k, side):
        sa, sb, da, db = halves(k)
        if side == 0:
            cp.got(("fa", k))
            fold(right, sa, fa)
            cp.add(("rla", k), part.at[c, right, da, :], rl.at[da, :], {"tensor": t_right}, ("rs", k))
        else:
            cp.got(("fb", k))
            fold(left, sb, fb)
            cp.add(("rrb", k), part.at[c, left, db, :], rr.at[db, :], {"tensor": t_left}, ("rs", k))

    def tcols(q):
        return pl.ds(pl.multiple_of(q * 128, 128), 128)

    def h_copy(name, rows, q, device, group=None):
        ref = hh.at[:, rows, tcols(q)]
        cp.add(name, ref, ref, {"tensor": device}, group)

    def activate(k):
        sa, sb, da, db = halves(k)
        for o, half in units_in(k):
            if o != 0 and o not in blocks_seen:
                blocks_seen.add(o)
                cp.got(("pr", (-o) % 8))
                col = to_col(prr[POS[o]][0:1, :])
                for i in range(2):
                    pcol[ROW[o, i] : ROW[o, i] + HALF, :] = col[i * HALF : (i + 1) * HALF, :]
        cp.got(("d", k, 0))
        sums = []
        cp.got_all(("rs", k), dbuf.at[pl.ds(0, 2), pl.ds(*rows_in(k)), :], {"tensor": t_sib})
        for s in (sb, sa):
            v = part[c, x, s, :].astype(F32) + dbuf[x, s, :].astype(F32)
            v = v + rl[s, :].astype(F32) + rr[s, :].astype(F32)
            gate, up, ga = v[:, 0:128], v[:, 128:256], v[:, 256:384]
            g = jax.nn.sigmoid(gate)
            hid = (gate * g * up).astype(BF16)
            a = pcol[s, :] * ga
            hh[0, s, tcols(t)] = hid
            hh[1, s, tcols(t)] = (a * up * g * (1.0 + gate * (1.0 - g))).astype(BF16)
            hh[2, s, tcols(t)] = (a * gate * g).astype(BF16)
            sums.insert(0, jnp.sum(hid.astype(F32) * ga, axis=1, keepdims=True))
        h_copy(("ra", k), da, t, t_right)
        h_copy(("lb", k), db, t, t_left)
        h_copy(("rb", k), db, t, t_right)
        h_copy(("la", k), da, t, t_left)
        h_copy(("so", k), pl.ds(*rows_in(k)), t, t_sib, ("s", k))
        dcol[sa, :] = sums[0]
        dcol[sb, :] = sums[1]
        for o, half in units_in(k):
            halves_seen.add((o, half))
            if (o, 1 - half) in halves_seen:
                col = jnp.concatenate(
                    [dcol[ROW[o, i] : ROW[o, i] + HALF, :] for i in range(2)], axis=0)
                p = POS[o]
                dps[p] = jnp.broadcast_to(to_row(col), (8, 128))
                if o != 0:
                    cp.add(("dp", o), dps.at[p], dpr.at[place(-o)], {"dp": (z + o) % 8}, "dp")
        r0, r = rows_in(k)
        s = slice(r0, r0 + r)
        sc[s, :] = (pcol[s, :] * gr[s, :].astype(F32)).astype(BF16)

    def spread(k, i):
        sa, sb, da, db = halves(k)
        full = pl.ds(*rows_in(k))
        if i == 0:
            cp.got(("ra", k))
            h_copy(("xa", k), da, t_left, t_right, ("x", k))
        if i == 1:
            cp.got(("lb", k))
            h_copy(("xb", k), db, t_right, t_left, ("x", k))
        if i == 2:
            cp.got(("rb", k))
            h_copy(("sl", k), full, t_left, t_sib, ("s", k))
        if i == 3:
            cp.got(("la", k))
            h_copy(("sr", k), full, t_right, t_sib, ("s", k))
        if i == 4:
            cp.got_all(("x", k), hh.at[:, full, pl.ds(0, 128)], {"tensor": t_sib})
            h_copy(("sx", k), full, across * 2 + c, t_sib, ("s", k))

    def tables(p):
        o = BLOCKS[p]
        if o != 0:
            cp.got(("ix", (-o) % 8))
        v = ix[p]
        both = table(v[0:1, :], v[2:3, :]) + table(v[1:2, :], v[3:4, :])
        selt[p] = both.T.astype(BF16)

    def chunks_in(m):
        k0, n = BACKS[m]
        return range(k0, k0 + n)

    def blocks_in(m):
        return [o for k in chunks_in(m) for o, half in units_in(k) if half == 0]

    def backward(m):
        for k in chunks_in(m):
            cp.got_all(("s", k), hh.at[:, pl.ds(*rows_in(k)), pl.ds(0, 512)], {"tensor": t_sib})
        r0 = rows_in(chunks_in(m)[0])[0]
        r = sum(rows_in(k)[1] for k in chunks_in(m))
        a = hh[1, r0 : r0 + r, :]
        b = hh[2, r0 : r0 + r, :]
        for i in range(3):
            cols = slice(i * 256, i * 256 + 256)
            dxs[r0 : r0 + r, cols] = (dot_nt(a, gw[cols, :]) + dot_nt(b, uw[cols, :])).astype(BF16)
        for i, o in enumerate(blocks_in(m)):
            v = jnp.concatenate([dxs[ROW[o, h] : ROW[o, h] + HALF, :] for h in range(2)], axis=0)
            yd[m][i] = dot_nn(selt[POS[o]], v).astype(BF16)

        if m in DIRECT:
            for q, put in ((2, yx[m]), (1, yr[m]), (3, yl[m])):
                rows = pl.ds(pl.multiple_of(((y + q) % 4) * 32, 32), 32)
                cp.add(("y", m, q), yd[m].at[:, rows, :], put, {"expert": (y + q) % 4}, ("yy", m))
            return

        def piece(q, low):
            return yd[m].at[:, pl.ds(pl.multiple_of(((y + q) % 4) * 32 + low, 16), 16), :]

        cp.add(("ya", m), piece(2, 0), ya[m], {"expert": (y + 1) % 4})
        cp.add(("yb", m), piece(2, 16), yb[m], {"expert": (y + 3) % 4})
        cp.add(("yr", m), piece(1, 16), yr[m].at[:, pl.ds(16, 16), :], {"expert": (y + 1) % 4},
               ("yy", m))
        cp.add(("yl", m), piece(3, 0), yl[m].at[:, pl.ds(0, 16), :], {"expert": (y + 3) % 4},
               ("yy", m))

    def relay(m):
        for name, q, low, buf, put in (("ya", 1, 0, ya, yr), ("yb", 3, 16, yb, yl)):
            cp.got((name, m))
            rows = pl.ds(pl.multiple_of(((y + q) % 4) * 32 + low, 16), 16)
            for i in range(len(blocks_in(m))):
                yd[m][i, rows, :] = (
                    yd[m][i, rows, :].astype(F32) + buf[m][i].astype(F32)).astype(BF16)
            cp.add((name, m, 2), yd[m].at[:, rows, :], put[m].at[:, pl.ds(low, 16), :],
                   {"expert": (y + q) % 4}, ("yy", m))

    def homeward(m):
        n = len(blocks_in(m))
        cp.got_all(("yy", m), yd[m].at[pl.ds(0, n), pl.ds(0, 96 if m in DIRECT else 64), :],
                   {"expert": (y + 1) % 4})
        rows = pl.ds(pl.multiple_of(y * 32, 32), 32)
        for i, o in enumerate(blocks_in(m)):
            v = yd[m][i, rows, :].astype(F32) + yr[m][i].astype(F32) + yl[m][i].astype(F32)
            if m in DIRECT:
                v = v + yx[m][i].astype(F32)
            if o == 0:
                own_q[...] = v
            else:
                yq[POS[o]] = v.astype(BF16)
                cp.add(("z", o), yq.at[POS[o]], zq.at[place(-o)], {"dp": (z + o) % 8}, "z")

    def router_1():
        total = dps[0][0:1, :]
        cp.got_all("dp", dpr.at[pl.ds(1, 7)], {"dp": (z + 1) % 8})
        for p in range(1, 8):
            total = total + dpr[p][0:1, :]
        col = to_col(total)
        pts[...] = rows8(jnp.sum(table0 * col, axis=0, keepdims=True),
                         jnp.sum(table1 * col, axis=0, keepdims=True))
        for k in range(1, 32):
            cp.add(("pt", k), pts, ptr.at[k],
                   {"expert": (y + k // 8) % 4, "tensor": (t + k) % 8}, "pt")

    def router_3():
        total = pts[...]
        cp.got_all("pt", ptr.at[pl.ds(1, 31)], {"tensor": t_sib})
        for k in range(1, 32):
            total = total + ptr[k]
        d0, d1 = total[0:1, :], total[1:2, :]
        p0, p1 = picks
        mixed = p0 * d0 + p1 * d1
        w0 = p0 * (d0 - mixed)
        w1 = p1 * (d1 - mixed)
        grads = [jnp.where(e0 == j, w0, 0.0) + jnp.where(e1 == j, w1, 0.0) for j in range(4)]
        split = [parts3(v) for v in grads]
        row = lax.broadcasted_iota(jnp.int32, (16, 128), 0)
        lhs = jnp.zeros((16, 128), F32)
        for i in range(3):
            for j in range(4):
                lhs = jnp.where(row == i * 4 + j, split[j][i].astype(F32), lhs)
        v = dot_nn(lhs.astype(BF16), tok_in[...])
        rgs[...] = v[0:4, :] + v[4:8, :] + v[8:12, :]
        for k in range(1, 8):
            cp.add(("rg", k), rgs, rgr.at[k], {"dp": (z + k) % 8}, "rg")
        i0 = lax.broadcasted_iota(jnp.int32, (128, 128), 0)
        i1 = lax.broadcasted_iota(jnp.int32, (128, 128), 1)
        eye_t = (i0 == i1).astype(F32)

        def col_t(row):
            return jnp.sum(eye_t * row, axis=1, keepdims=True)

        lane = lax.broadcasted_iota(jnp.int32, (128, 16), 1)
        of_expert = (lane % 4).astype(F32)
        v = (jnp.where(col_t(e0.astype(F32)) == of_expert, col_t(w0), 0.0)
             + jnp.where(col_t(e1.astype(F32)) == of_expert, col_t(w1), 0.0))
        hi, mid, low = (q.astype(F32) for q in parts3(v))
        lg3[...] = jnp.where(lane < 4, hi, jnp.where(lane < 8, mid, jnp.where(lane < 12, low, 0.0)))

    def router_5():
        total = rgs[...]
        cp.got_all("rg", rgr.at[pl.ds(1, 7)], {"dp": (z + 1) % 8})
        for k in range(1, 8):
            total = total + rgr[k]
        router_out[...] = total

    def finish():
        cp.drain()
        many = ptr.at[pl.ds(1, 31)]
        cp.describe("pt", many, many, {"tensor": t_sib}, N_SEND).wait_send()
        rows = pl.ds(pl.multiple_of(y * 32, 32), 32)
        total = own_q[...]
        total = total + dot_nn(lg3[rows, :].astype(BF16), jnp.concatenate([rwt[...]] * 4, axis=0))
        cp.got_all("z", zq.at[pl.ds(1, 7)], {"dp": (z + 1) % 8})
        for p in range(1, 8):
            total = total + zq[p].astype(F32)
        tok_out[...] = total.astype(BF16)

    def weights(m, i):
        out, left_side, right_side = (
            (gg_o, tk, hh.at[1]), (ug_o, tk, hh.at[2]), (dg_o, hh.at[0], sc))[m]
        size = out.shape[0] // 3 if m < 2 else out.shape[0] // 4
        rows = slice(i * size, i * size + size)
        out[rows, :] = lax.dot_general(
            left_side[:, rows], right_side[...], (((0,), (0,)), ((), ())),
            preferred_element_type=F32).astype(BF16)

    run = {
        "open": open_up, "prob": probabilities, "far": far, "Z": pass_on, "F": forward, "D": to_sibling,
        "R1": reduce_1, "R2": reduce_2, "E": activate, "G": spread, "X": backward,
        "Y": homeward, "P1": router_1, "P3": router_3,
        "P5": router_5, "S": tables, "V": relay, "W": weights, "end": finish,
    }
    for step in STEPS:
        run[step[0]](*step[1:])


def put_out(*refs):
    sem = refs[10]
    copies = [pltpu.make_async_copy(refs[i], refs[5 + i], sem.at[i]) for i in range(5)]
    for q in copies:
        q.start()
    for q in copies:
        q.wait()


def shards(
    tokens, out_grad, router_weight, gate_weight, up_weight, down_weight, expert_index, slot_index
):
    vm = pl.BlockSpec(memory_space=pltpu.VMEM)
    hbm = pl.BlockSpec(memory_space=pltpu.HBM)
    V = pltpu.VMEM
    small = V((8, 128), F32)
    several = V((8, 8, 128), F32)
    out_shape = [
        jax.ShapeDtypeStruct((32, 768), BF16),
        jax.ShapeDtypeStruct((4, 768), F32),
        jax.ShapeDtypeStruct((768, 1024), BF16),
        jax.ShapeDtypeStruct((768, 1024), BF16),
        jax.ShapeDtypeStruct((1024, 768), BF16),
    ]
    results = pl.pallas_call(
        kernel,
        name="moe_backward",
        in_specs=[hbm] * 8,
        out_specs=[vm] * 5,
        out_shape=out_shape,
        scratch_shapes=[
            V((768, 768), BF16), V((768, 768), BF16), V((768, 768), BF16),
            V((768, 1024), BF16), V((768, 1024), BF16), V((1024, 768), BF16),
            V((2, 4, 768, 384), BF16), V((4, 768, 384), BF16),
            V((768, 384), BF16), V((768, 384), BF16), V((768, 384), BF16), V((768, 384), BF16),
            V((3, 768, 1024), BF16), V((768, 1), F32), V((768, 1), F32),
            small, several, small, several, several, several, V((8, 8, 128), jnp.int32),
            V((8, 128, CAP), BF16), V((768, 768), BF16), V((8, 32, 768), BF16),
            V((8, 32, 768), BF16), V((32, 768), F32),
            small, V((32, 8, 128), F32), V((4, 768), F32), V((8, 4, 768), F32), V((128, 16), F32),
            V((128, 768), BF16), V((128, 768), BF16), V((4, 768), BF16),
            V((2, 128), jnp.int32), V((2, 128), jnp.int32),
            pltpu.SemaphoreType.DMA((N_SEND + 1,)), pltpu.SemaphoreType.DMA((N_RECV,)),
            pltpu.SemaphoreType.DMA((8,)),
            *(V((sum(GROUPS[k0 : k0 + n]) // 2, rows, 768), BF16)
              for rows in (128, 16, 16, 32, 32, 32) for k0, n in BACKS),
        ],
        compiler_params=pltpu.CompilerParams(
            collective_id=0, has_side_effects=True, vmem_limit_bytes=40 * 1024 * 1024
        ),
    )(
        *(pltpu.with_memory_space_constraint(v, pltpu.HBM) for v in (
            tokens, out_grad, router_weight.T, expert_index.T, slot_index.T,
            gate_weight[0], up_weight[0], down_weight[0],
        ))
    )
    tokens_grad, router_grad, gate_grad, up_grad, down_grad = pl.pallas_call(
        put_out,
        name="put_out",
        in_specs=[vm] * 5,
        out_specs=[hbm] * 5,
        out_shape=out_shape,
        scratch_shapes=[pltpu.SemaphoreType.DMA((5,))],
        compiler_params=pltpu.CompilerParams(vmem_limit_bytes=1024 * 1024),
    )(*results)
    return (tokens_grad, router_grad.T, gate_grad[None], up_grad[None], down_grad[None])


def solution(mesh):
    in_specs = (
        P("dp", "tensor"),
        P("dp", "tensor"),
        P("tensor", None),
        P("expert", "tensor", "dp"),
        P("expert", "tensor", "dp"),
        P("expert", "dp", "tensor"),
        P("dp", None),
        P("dp", None),
    )
    out_specs = (
        P(("dp", "expert"), "tensor"),
        P("tensor", None),
        P("expert", "tensor", "dp"),
        P("expert", "tensor", "dp"),
        P("expert", "dp", "tensor"),
    )
    return jax.shard_map(shards, mesh=mesh, in_specs=in_specs, out_specs=out_specs, check_vma=False)
```
